32 devices in a mesh: band: 8 (over z, y), grid: 4 (over x, core).
Axes of the slice: x: 2, y: 2, z: 4, core: 2. Of those that a mesh axis runs over, the one named last changes fastest.
Arguments:
- own_bands: float32 [32, 128, 128, 128], P('band', 'grid'), may hold values from -1.5 to 1.5
- travel_bands: float32 [32, 128, 128, 128], P('band', 'grid'), may hold values from -1.5 to 1.5
Outputs:
- own_terms: float32 [32, 128, 128, 128], P('band', 'grid')
- partner_terms: float32 [32, 128, 128, 128], P('band', 'grid')
The draws below stay inside these ranges and needn't reach their ends.
All inputs are finite; a program needn't handle non-finite values.
Results may differ from the reference program's by a relative error of at most 0.00011.
Values sent between devices are 32-bit elements; how exact they have to be, the bound alone decides.
A program may use at most 192 MiB of HBM per device.

```python
import math
import jax
import jax.numpy as jnp
from jax import lax

NX = 128
NY = 128
NZ = 128
OWN = 4
VIS = 4
BANDS = 32
TRAVEL = 32
N_BAND = 8


def band_field(base_key, band_count):
    return 0.5 * jax.random.truncated_normal(jax.random.fold_in(base_key, 4), -3.0, 3.0, (band_count, NZ, NY, NX), jnp.float32)


def draw_own_bands(key, part):
    return band_field(jax.random.fold_in(key, 11), BANDS)


def draw_travel_bands(key, part):
    return band_field(jax.random.fold_in(key, 23), TRAVEL)


def setup_inputs(seed: int = 0) -> dict:
    streams_of = jax.random.split(jax.random.key(seed), 3)
    return {
        "own_bands": draw_own_bands(jax.random.fold_in(streams_of[2], 71), 0),
        "travel_bands": draw_travel_bands(jax.random.fold_in(streams_of[2], 71), 0),
    }


FRACTION = 0.25


def wave_square(points, first_row, length):
    position = first_row + jnp.arange(points, dtype=jnp.int32)
    position = (position + length // 2) % length - length // 2
    wavenumber = (2.0 * math.pi / length) * position.astype(jnp.float32)
    return wavenumber * wavenumber


def coulomb(first_row, row_count):
    squared = wave_square(NZ, 0, NZ)[:, None, None] + wave_square(row_count, first_row, NY)[None, :, None] + wave_square(NX, 0, NX)[None, None, :]
    safe_square = jnp.where(squared > 0.0, squared, 1.0)
    return jnp.where(squared > 0.0, 4.0 * math.pi / safe_square, 0.0)


def reference(own_bands, travel_bands):
    kernel = coulomb(0, NY)[:, :, : NX // 2 + 1]
    owned_groups = own_bands.reshape(N_BAND, OWN, NZ, NY, NX)
    arrived = jnp.roll(travel_bands.reshape(N_BAND, VIS, NZ, NY, NX), 1, axis=0)

    def group_terms(blocks):
        owned, visitors = blocks

        def visit_band(accumulated, visitor):
            density = owned * visitor
            potential = jnp.fft.irfftn(kernel * jnp.fft.rfftn(density, axes=(1, 2, 3)), s=(NZ, NY, NX), axes=(1, 2, 3))
            return accumulated + potential * visitor, jnp.sum(potential * owned, axis=0)

        accumulated, partner = lax.scan(visit_band, jnp.zeros_like(owned), visitors)
        return -FRACTION * accumulated, -FRACTION * partner

    own_terms, held = lax.map(group_terms, (owned_groups, arrived))
    held = jnp.roll(held, -1, axis=0)
    return own_terms.reshape(BANDS, NZ, NY, NX), held.reshape(TRAVEL, NZ, NY, NX)
```

```python
import functools
import math

import jax
import jax.numpy as jnp
import numpy as np
from jax import lax
from jax.experimental import pallas as pl
from jax.experimental.pallas import tpu as pltpu
from jax.sharding import PartitionSpec as P


FRACTION = 0.25
HIGHEST_PRECISION = lax.Precision.HIGHEST
CHUNK = 8


def passed_along(block, axis, distance):
    devices = range(lax.axis_size(axis))
    route = [((i - distance) % len(devices), i) for i in devices]
    return lax.ppermute(block, axis, route)


def wave_square(points, first_row, length):
    position = first_row + jnp.arange(points, dtype=jnp.int32)
    return squared_wavenumber(position, length)


def squared_wavenumber(position, length):
    position = (position + length // 2) % length - length // 2
    wavenumber = 2.0 * math.pi / length * position.astype(jnp.float32)
    return wavenumber * wavenumber


def coulomb(square_z, square_y, square_x):
    squared = square_z[:, None, None] + square_y[None, :, None] + square_x[None, None, :]
    safe_square = jnp.where(squared > 0.0, squared, 1.0)
    return jnp.where(squared > 0.0, 4.0 * math.pi / safe_square, 0.0)


def fourier_table(length, inverse):
    position = jnp.arange(length, dtype=jnp.int32)
    phase_turns = position[:, None] * position[None, :] % length
    phase_angle = 2.0 * math.pi / length * phase_turns.astype(jnp.float32)
    cosine = jnp.cos(phase_angle)
    sine_part = jnp.sin(phase_angle)
    norm_factor = 1.0
    if inverse:
        sine_part = -sine_part
        norm_factor = 1.0 / length
    return norm_factor * jnp.stack(
        [jnp.stack([cosine, -sine_part]), jnp.stack([sine_part, cosine])]
    )


def solve_pairs(packed, kernel_slab, nz):
    ny, nx = packed.shape[3:]
    spectrum = jnp.einsum(
        "pczyx,cdxk->dpzyk", packed, fourier_table(nx, False), precision=HIGHEST_PRECISION
    )
    spectrum = jnp.einsum(
        "cpzyx,cdyk->dpzkx", spectrum, fourier_table(ny, False), precision=HIGHEST_PRECISION
    )
    forward_z = fourier_table(nz, False)
    inverse_z = fourier_table(nz, True)
    screened = (
        jnp.einsum(
            "cpzyx,cdzk->dpkyx",
            lax.all_to_all(spectrum, "grid", split_axis=3, concat_axis=2, tiled=True),
            forward_z,
            precision=HIGHEST_PRECISION,
        )
        * kernel_slab
    )
    screened = jnp.einsum("cpzyx,cdzk->dpkyx", screened, inverse_z, precision=HIGHEST_PRECISION)
    planes = lax.all_to_all(screened, "grid", split_axis=2, concat_axis=3, tiled=True)
    planes = jnp.einsum(
        "cpzyx,cdyk->dpzkx", planes, fourier_table(ny, True), precision=HIGHEST_PRECISION
    )
    return jnp.einsum(
        "cpzyx,cdxk->pdzyk", planes, fourier_table(nx, True), precision=HIGHEST_PRECISION
    )


def pair_terms(owned, visitors, kernel_slab, nz):
    count_vis = visitors.shape[0]
    count_own = owned.shape[0]
    density = owned[None] * visitors[:, None]
    packed = density.reshape((count_vis * count_own // 2, 2) + owned.shape[1:])
    potential = solve_pairs(packed, kernel_slab, nz).reshape(density.shape)
    own_part = jnp.sum(potential * visitors[:, None], axis=0)
    partner = jnp.sum(potential * owned[None], axis=1)
    return (own_part, partner)


def body(own_bands, travel_bands):
    depth, ny, nx = own_bands.shape[1:]
    nz = depth * lax.axis_size("grid")
    rows_local = ny // lax.axis_size("grid")
    kernel_slab = coulomb(
        wave_square(nz, 0, nz),
        wave_square(rows_local, lax.axis_index("grid") * rows_local, ny),
        wave_square(nx, 0, nx),
    )
    count_vis = travel_bands.shape[0]
    own_total = jnp.zeros_like(own_bands)
    returned = []
    for visit_index in range(count_vis):
        visitor = passed_along(travel_bands[visit_index : visit_index + 1], "band", 1)
        own_part, partner = pair_terms(own_bands, visitor, kernel_slab, nz)
        own_total = own_total + own_part
        returned.append(passed_along(partner, "band", -1))
    partner_total = jnp.concatenate(returned, axis=0)
    return (-FRACTION * own_total, -FRACTION * partner_total)


def halves(table):
    high = table.astype(jnp.bfloat16)
    return high, (table - high.astype(np.float32)).astype(jnp.bfloat16)


def complex_matrix(length, inverse, left):
    position = np.arange(length)
    angle = 2.0 * np.pi / length * (position[:, None] * position[None, :] % length)
    cosine, sine = np.cos(angle), np.sin(angle)
    if inverse:
        sine = -sine
    matrix = np.block([[cosine, -sine], [sine, cosine]])
    return (matrix.T if left else matrix).astype(np.float32)


def times(value, factor):
    (a, b), (c, d) = value, factor
    if abs(d) < 1e-12:
        return (a, b) if c > 0.5 else (-a, -b)
    if abs(c) < 1e-12:
        return (-b, a) if d > 0.0 else (b, -a)
    if abs(abs(c) - abs(d)) < 1e-12:
        size = abs(c)
        first = a if c > 0 else -a
        other = b if c > 0 else -b
        if (c > 0) == (d > 0):
            return size * (first - other), size * (first + other)
        return size * (first + other), size * (other - first)
    return a * c - b * d, a * d + b * c


def turn(numerator, length, sign):
    angle = 2.0 * math.pi * (numerator % length) / length
    return math.cos(angle), sign * math.sin(angle)


def fourier(values, sign):
    count = len(values)
    if count == 1:
        return values
    half = count // 2
    sums, differences = [], []
    for i in range(half):
        (a, b), (c, d) = values[i], values[i + half]
        sums.append((a + c, b + d))
        differences.append(times((a - c, b - d), turn(i, count, sign)))
    even = fourier(sums, sign)
    odd = fourier(differences, sign)
    return [pair for both in zip(even, odd) for pair in both]


def split(value):
    high = value.astype(jnp.bfloat16)
    return high, (value - high.astype(jnp.float32)).astype(jnp.bfloat16)


def dot(a, b):
    return jnp.dot(a, b, preferred_element_type=jnp.float32)


def product(left, right):
    (a, b), (c, d) = left, right
    return dot(a, c) + dot(b, c) + dot(a, d)


def field_kernel(radix, first_call, rank_ref, *refs):
    refs = list(refs)

    def take(count):
        taken = refs[:count]
        del refs[:count]
        return taken

    own_hbm, vis_hbm = take(4), take(4)
    (weights_hbm,) = take(1)
    tables = take(8)
    before_hbm = [] if first_call else take(2)
    held_hbm, sums_hbm = take(2), take(2)
    own_ref, vis_ref, real_ref, imag_ref, weights_ref, total_ref = take(6)
    own_sem, vis_sem, weights_sem, before_sem, held_sem, sums_sem = refs
    nz, ny, nx = real_ref.shape
    depth = nz // 4
    rank = rank_ref[0]

    def planes(slot):
        return pl.ds(lax.bitwise_xor(rank, slot) * depth, depth)

    own_in, vis_in, before_in, held_out, sums_out = [], [], [], [], []
    for s in range(4):
        own_in.append(
            pltpu.make_async_copy(own_hbm[s], own_ref.at[:, planes(s)], own_sem.at[s])
        )
        vis_in.append(pltpu.make_async_copy(vis_hbm[s], vis_ref.at[planes(s)], vis_sem.at[s]))
    weights_in = pltpu.make_async_copy(weights_hbm, weights_ref, weights_sem)
    for s in range(2):
        part = total_ref.at[:, pl.ds(s * depth, depth)]
        if not first_call:
            before_in.append(pltpu.make_async_copy(before_hbm[s], part, before_sem.at[s]))
        sums_out.append(pltpu.make_async_copy(part, sums_hbm[s], sums_sem.at[s]))
        held_out.append(
            pltpu.make_async_copy(vis_ref.at[planes(s)], held_hbm[s], held_sem.at[s])
        )
    for copy in [c for both in zip(own_in, vis_in) for c in both] + [weights_in] + before_in:
        copy.start()

    def loaded(index):
        return tables[index][...], tables[index + 1][...]

    def forward(z):
        visitor = vis_ref[pl.ds(z, 2)]
        real = (own_ref[0, pl.ds(z, 2)] * visitor).reshape(2 * ny, nx)
        imag = (own_ref[1, pl.ds(z, 2)] * visitor).reshape(2 * ny, nx)
        rows = jnp.concatenate([real, imag], axis=1)
        rows = product(split(rows), loaded(0))
        columns = jnp.concatenate(
            [
                jnp.concatenate([rows[:ny, :nx], rows[ny:, :nx]], axis=1),
                jnp.concatenate([rows[:ny, nx:], rows[ny:, nx:]], axis=1),
            ],
            axis=0,
        )
        columns = product(loaded(2), split(columns))
        for i in (0, 1):
            real_ref[z + i] = columns[:ny, i * nx : (i + 1) * nx]
            imag_ref[z + i] = columns[ny:, i * nx : (i + 1) * nx]

    def backward(z, kept):
        columns = jnp.concatenate(
            [
                jnp.concatenate([ref[z], ref[z + 1]], axis=1)
                for ref in (real_ref, imag_ref)
            ],
            axis=0,
        )
        columns = product(loaded(4), split(columns))
        rows = jnp.concatenate(
            [
                jnp.concatenate([columns[:ny, :nx], columns[ny:, :nx]], axis=1),
                jnp.concatenate([columns[:ny, nx:], columns[ny:, nx:]], axis=1),
            ],
            axis=0,
        )
        rows = product(split(rows), loaded(6))
        real = rows[:, :nx].reshape(2, ny, nx)
        imag = rows[:, nx:].reshape(2, ny, nx)
        visitor = vis_ref[pl.ds(z, 2)]
        vis_ref[pl.ds(z, 2)] = real * own_ref[0, pl.ds(z, 2)] + imag * own_ref[1, pl.ds(z, 2)]
        for i, part in enumerate((real, imag)):
            part = part * visitor
            if not first_call:
                part = part + total_ref[i, pl.ds(kept, 2)]
            total_ref[i, pl.ds(kept, 2)] = part

    def tile(index, carry):
        here = pl.ds(pl.multiple_of(8 * index, 8), 8)
        outer = nz // radix

        def load(z):
            return real_ref[z, here, :], imag_ref[z, here, :]

        def store(z, value):
            real_ref[z, here, :], imag_ref[z, here, :] = value

        for fine in range(radix):
            values = fourier([load(radix * n + fine) for n in range(outer)], -1.0)
            for k, value in enumerate(values):
                store(radix * k + fine, times(value, turn(fine * k, nz, -1.0)))
        for k in range(outer):
            values = fourier([load(radix * k + n) for n in range(radix)], -1.0)
            for n, (a, b) in enumerate(values):
                weight = weights_ref[radix * k + n, here, :]
                values[n] = (a * weight, b * weight)
            for n, value in enumerate(fourier(values, 1.0)):
                store(radix * k + n, value)
        for fine in range(radix):
            values = [times(load(radix * k + fine), turn(fine * k, nz, 1.0)) for k in range(outer)]
            for n, value in enumerate(fourier(values, 1.0)):
                store(radix * n + fine, value)
        return carry

    def forward_slot(s, carry):
        here = planes(s)
        pltpu.make_async_copy(own_hbm[0], own_ref.at[:, here], own_sem.at[s]).wait()
        pltpu.make_async_copy(vis_hbm[0], vis_ref.at[here], vis_sem.at[s]).wait()
        base = lax.bitwise_xor(rank, s) * depth

        def forward_chunk(chunk, carry):
            for pair in range(CHUNK // 2):
                forward(base + chunk * CHUNK + 2 * pair)
            return carry

        return lax.fori_loop(0, depth // CHUNK, forward_chunk, carry)

    lax.fori_loop(0, 4, forward_slot, 0)
    weights_in.wait()
    lax.fori_loop(0, ny // 8, tile, 0)
    for s in (1, 0):
        if not first_call:
            before_in[s].wait()
        base = lax.bitwise_xor(rank, s) * depth

        def backward_chunk(chunk, carry):
            for pair in range(CHUNK // 2):
                offset = chunk * CHUNK + 2 * pair
                backward(base + offset, s * depth + offset)
            return carry

        lax.fori_loop(0, depth // CHUNK, backward_chunk, 0)
        held_out[s].start()
        sums_out[s].start()
    for copy in held_out + sums_out:
        copy.wait()


def solve_field(rank, owned, visitor, weights, tables, before):
    depth, ny, nx = visitor[0].shape
    nz = 4 * depth
    first_call = before is None
    operands = list(owned) + list(visitor) + [weights] + list(tables)
    anywhere = pl.BlockSpec(memory_space=pl.ANY)
    in_specs = [pl.BlockSpec(memory_space=pltpu.SMEM)] + [anywhere] * 9
    in_specs += [pl.BlockSpec(memory_space=pltpu.VMEM)] * 8
    if not first_call:
        in_specs += [anywhere] * 2
        operands += list(before)
    shapes = [jax.ShapeDtypeStruct(v.shape, v.dtype) for v in visitor[:2]]
    shapes += [jax.ShapeDtypeStruct(v.shape, v.dtype) for v in owned[:2]]
    points = nz * ny * nx
    grid = pltpu.VMEM((nz, ny, nx), jnp.float32)
    results = pl.pallas_call(
        functools.partial(field_kernel, 8, first_call),
        out_shape=shapes,
        in_specs=in_specs,
        out_specs=[anywhere] * 4,
        scratch_shapes=[
            pltpu.VMEM((2, nz, ny, nx), jnp.float32),
            grid,
            grid,
            grid,
            grid,
            pltpu.VMEM((2, 2 * depth, ny, nx), jnp.float32),
            pltpu.SemaphoreType.DMA((4,)),
            pltpu.SemaphoreType.DMA((4,)),
            pltpu.SemaphoreType.DMA,
            pltpu.SemaphoreType.DMA((2,)),
            pltpu.SemaphoreType.DMA((2,)),
            pltpu.SemaphoreType.DMA((2,)),
        ],
        compiler_params=pltpu.CompilerParams(vmem_limit_bytes=67043328),
        cost_estimate=pl.CostEstimate(
            flops=2 * points * 3 * 4 * nx, bytes_accessed=4 * points * 10, transcendentals=0
        ),
        name="solve_field",
    )(rank, *operands)
    return results[:2], results[2:]


def exchanged(block, bit):
    devices = range(lax.axis_size("grid"))
    return lax.ppermute(block, "grid", [(i, i ^ bit) for i in devices])


def picked(bands, first, count):
    return lax.dynamic_slice_in_dim(bands, first, count, 0)


def square_body(own_bands, travel_bands):
    rank = lax.axis_index("grid")
    core = rank % 2
    half_own = own_bands.shape[0] // 2
    count_vis = travel_bands.shape[0]
    depth, ny, nx = own_bands.shape[1:]
    nz = depth * lax.axis_size("grid")

    own_mine = picked(own_bands, core * half_own, half_own)
    own_far = exchanged(own_mine, 2)
    own_bands, travel_bands, _ = lax.optimization_barrier((own_bands, travel_bands, own_mine))
    own_side = exchanged(picked(own_bands, (1 - core) * half_own, half_own), 1)
    own_cross = exchanged(own_side, 2)
    owned = [own_mine, own_side, own_far, own_cross]

    visitors = []
    for j in range(count_vis):
        near = passed_along(travel_bands[j], "band", 1)
        far = exchanged(near, 2)
        side = exchanged(near, 1)
        cross = exchanged(far, 1)
        visitors.append([near, side, far, cross])

    radix = 8
    slot = jnp.arange(nz, dtype=jnp.int32)
    z_of_slot = slot // radix + (nz // radix) * (slot % radix)
    weights = (-FRACTION / (nz * ny * nx)) * coulomb(
        squared_wavenumber(z_of_slot, nz), wave_square(ny, 0, ny), wave_square(nx, 0, nx)
    )
    tables = []
    for length, inverse, left in (
        (nx, False, False),
        (ny, False, True),
        (ny, True, True),
        (nx, True, False),
    ):
        tables += halves(complex_matrix(length, inverse, left))
    rank_operand = rank.astype(jnp.int32).reshape(1)

    sums = None
    returned = []
    for j in range(count_vis):
        held, sums = solve_field(rank_operand, owned, visitors[j], weights, tables, sums)
        other = exchanged(held[1], 1)
        returned.append(passed_along(held[0] + other, "band", -1))
    held_rows = jnp.stack(returned)

    own_other = exchanged(sums[1], 1)
    own_rows = jnp.zeros(own_bands.shape, own_bands.dtype)
    own_rows = lax.dynamic_update_slice_in_dim(own_rows, sums[0], core * half_own, 0)
    own_rows = lax.dynamic_update_slice_in_dim(own_rows, own_other, (1 - core) * half_own, 0)
    return own_rows, held_rows


def whole_body(own_bands, travel_bands):
    return square_body(own_bands, travel_bands)


def solution(mesh):
    spec = P("band", "grid", None, None)

    def placed(own_bands, travel_bands):
        group_own = own_bands.shape[0] // mesh.shape["band"]
        group_vis = travel_bands.shape[0] // mesh.shape["band"]
        square = mesh.shape["grid"] == 4 and group_own == 4 and group_vis % 2 == 0
        step = jax.shard_map(
            whole_body if square else body,
            mesh=mesh,
            in_specs=(spec, spec),
            out_specs=(spec, spec),
            check_vma=False,
        )
        return step(own_bands, travel_bands)

    return placed
```

```python
import functools
import math

import jax
import jax.numpy as jnp
import numpy as np
from jax import lax
from jax.experimental import pallas as pl
from jax.experimental.pallas import tpu as pltpu
from jax.sharding import PartitionSpec as P


FRACTION = 0.25
HIGHEST_PRECISION = lax.Precision.HIGHEST
CHUNK = 8


def passed_along(block, axis, distance):
    devices = range(lax.axis_size(axis))
    route = [((i - distance) % len(devices), i) for i in devices]
    return lax.ppermute(block, axis, route)


def wave_square(points, first_row, length):
    position = first_row + jnp.arange(points, dtype=jnp.int32)
    return squared_wavenumber(position, length)


def squared_wavenumber(position, length):
    position = (position + length // 2) % length - length // 2
    wavenumber = 2.0 * math.pi / length * position.astype(jnp.float32)
    return wavenumber * wavenumber


def coulomb(square_z, square_y, square_x):
    squared = square_z[:, None, None] + square_y[None, :, None] + square_x[None, None, :]
    safe_square = jnp.where(squared > 0.0, squared, 1.0)
    return jnp.where(squared > 0.0, 4.0 * math.pi / safe_square, 0.0)


def fourier_table(length, inverse):
    position = jnp.arange(length, dtype=jnp.int32)
    phase_turns = position[:, None] * position[None, :] % length
    phase_angle = 2.0 * math.pi / length * phase_turns.astype(jnp.float32)
    cosine = jnp.cos(phase_angle)
    sine_part = jnp.sin(phase_angle)
    norm_factor = 1.0
    if inverse:
        sine_part = -sine_part
        norm_factor = 1.0 / length
    return norm_factor * jnp.stack(
        [jnp.stack([cosine, -sine_part]), jnp.stack([sine_part, cosine])]
    )


def solve_pairs(packed, kernel_slab, nz):
    ny, nx = packed.shape[3:]
    spectrum = jnp.einsum(
        "pczyx,cdxk->dpzyk", packed, fourier_table(nx, False), precision=HIGHEST_PRECISION
    )
    spectrum = jnp.einsum(
        "cpzyx,cdyk->dpzkx", spectrum, fourier_table(ny, False), precision=HIGHEST_PRECISION
    )
    forward_z = fourier_table(nz, False)
    inverse_z = fourier_table(nz, True)
    screened = (
        jnp.einsum(
            "cpzyx,cdzk->dpkyx",
            lax.all_to_all(spectrum, "grid", split_axis=3, concat_axis=2, tiled=True),
            forward_z,
            precision=HIGHEST_PRECISION,
        )
        * kernel_slab
    )
    screened = jnp.einsum("cpzyx,cdzk->dpkyx", screened, inverse_z, precision=HIGHEST_PRECISION)
    planes = lax.all_to_all(screened, "grid", split_axis=2, concat_axis=3, tiled=True)
    planes = jnp.einsum(
        "cpzyx,cdyk->dpzkx", planes, fourier_table(ny, True), precision=HIGHEST_PRECISION
    )
    return jnp.einsum(
        "cpzyx,cdxk->pdzyk", planes, fourier_table(nx, True), precision=HIGHEST_PRECISION
    )


def pair_terms(owned, visitors, kernel_slab, nz):
    count_vis = visitors.shape[0]
    count_own = owned.shape[0]
    density = owned[None] * visitors[:, None]
    packed = density.reshape((count_vis * count_own // 2, 2) + owned.shape[1:])
    potential = solve_pairs(packed, kernel_slab, nz).reshape(density.shape)
    own_part = jnp.sum(potential * visitors[:, None], axis=0)
    partner = jnp.sum(potential * owned[None], axis=1)
    return (own_part, partner)


def body(own_bands, travel_bands):
    depth, ny, nx = own_bands.shape[1:]
    nz = depth * lax.axis_size("grid")
    rows_local = ny // lax.axis_size("grid")
    kernel_slab = coulomb(
        wave_square(nz, 0, nz),
        wave_square(rows_local, lax.axis_index("grid") * rows_local, ny),
        wave_square(nx, 0, nx),
    )
    count_vis = travel_bands.shape[0]
    own_total = jnp.zeros_like(own_bands)
    returned = []
    for visit_index in range(count_vis):
        visitor = passed_along(travel_bands[visit_index : visit_index + 1], "band", 1)
        own_part, partner = pair_terms(own_bands, visitor, kernel_slab, nz)
        own_total = own_total + own_part
        returned.append(passed_along(partner, "band", -1))
    partner_total = jnp.concatenate(returned, axis=0)
    return (-FRACTION * own_total, -FRACTION * partner_total)


def halves(table):
    high = table.astype(jnp.bfloat16)
    return high, (table - high.astype(np.float32)).astype(jnp.bfloat16)


def complex_matrix(length, inverse, left):
    position = np.arange(length)
    angle = 2.0 * np.pi / length * (position[:, None] * position[None, :] % length)
    cosine, sine = np.cos(angle), np.sin(angle)
    if inverse:
        sine = -sine
    matrix = np.block([[cosine, -sine], [sine, cosine]])
    return (matrix.T if left else matrix).astype(np.float32)


def times(value, factor):
    (a, b), (c, d) = value, factor
    if abs(d) < 1e-12:
        return (a, b) if c > 0.5 else (-a, -b)
    if abs(c) < 1e-12:
        return (-b, a) if d > 0.0 else (b, -a)
    if abs(abs(c) - abs(d)) < 1e-12:
        size = abs(c)
        first = a if c > 0 else -a
        other = b if c > 0 else -b
        if (c > 0) == (d > 0):
            return size * (first - other), size * (first + other)
        return size * (first + other), size * (other - first)
    return a * c - b * d, a * d + b * c


def turn(numerator, length, sign):
    angle = 2.0 * math.pi * (numerator % length) / length
    return math.cos(angle), sign * math.sin(angle)


def fourier(values, sign):
    count = len(values)
    if count == 1:
        return values
    half = count // 2
    sums, differences = [], []
    for i in range(half):
        (a, b), (c, d) = values[i], values[i + half]
        sums.append((a + c, b + d))
        differences.append(times((a - c, b - d), turn(i, count, sign)))
    even = fourier(sums, sign)
    odd = fourier(differences, sign)
    return [pair for both in zip(even, odd) for pair in both]


def split(value):
    high = value.astype(jnp.bfloat16)
    return high, (value - high.astype(jnp.float32)).astype(jnp.bfloat16)


def dot(a, b):
    return jnp.dot(a, b, preferred_element_type=jnp.float32)


def product(left, right):
    (a, b), (c, d) = left, right
    return dot(a, c) + dot(b, c) + dot(a, d)


def transform_planes(real, imag, x_table, y_table, inverse):
    _, ny, nx = real.shape

    def along_x(real, imag):
        rows = jnp.concatenate([part.reshape(2 * ny, nx) for part in (real, imag)], axis=1)
        rows = product(split(rows), x_table)
        return [rows[:, i * nx : (i + 1) * nx].reshape(2, ny, nx) for i in (0, 1)]

    def along_y(real, imag):
        columns = jnp.concatenate(
            [jnp.concatenate([part[0], part[1]], axis=1) for part in (real, imag)], axis=0
        )
        columns = product(y_table, split(columns))
        return [
            jnp.stack([columns[i * ny : (i + 1) * ny, p * nx : (p + 1) * nx] for p in (0, 1)])
            for i in (0, 1)
        ]

    if inverse:
        return along_x(*along_y(real, imag))
    return along_y(*along_x(real, imag))


def near_kernel(own_0, own_1, vis_0, vis_1, order, x_high, x_low, y_high, y_low, out, *scratch):
    own_ref, vis_ref, own_sem, vis_sem, out_sem = scratch
    depth = vis_0.shape[0]
    own_hbm, vis_hbm = (own_0, own_1), (vis_0, vis_1)
    copies = []
    for s in range(2):
        part = pl.ds(s * depth, depth)
        copies.append(
            [
                pltpu.make_async_copy(own_hbm[s], own_ref.at[:, part], own_sem.at[s]),
                pltpu.make_async_copy(vis_hbm[s], vis_ref.at[part], vis_sem.at[s]),
            ]
        )
        for copy in copies[s]:
            copy.start()
    x_table = x_high[...], x_low[...]
    y_table = y_high[...], y_low[...]

    def slot(s, carry):
        part = pl.ds(s * depth, depth)
        pltpu.make_async_copy(own_0, own_ref.at[:, part], own_sem.at[s]).wait()
        pltpu.make_async_copy(vis_0, vis_ref.at[part], vis_sem.at[s]).wait()

        def chunk(index, carry):
            start = s * depth + index * CHUNK
            for pair in range(CHUNK // 2):
                here = pl.ds(start + 2 * pair, 2)
                visitor = vis_ref[here]
                real, imag = transform_planes(
                    own_ref[0, here] * visitor, own_ref[1, here] * visitor, x_table, y_table, False
                )
                own_ref[0, here] = real
                own_ref[1, here] = imag
            here = pl.ds(start, CHUNK)
            pltpu.make_async_copy(own_ref.at[:, here], out.at[:, here], out_sem).start()
            return carry

        return lax.fori_loop(0, depth // CHUNK, chunk, carry)

    lax.fori_loop(0, 2, slot, 0)
    pltpu.make_async_copy(own_ref, out, out_sem).wait()


def near_field(owned, visitor, order, tables):
    depth, ny, nx = visitor[0].shape
    anywhere = pl.BlockSpec(memory_space=pl.ANY)
    points = 2 * depth * ny * nx
    return pl.pallas_call(
        near_kernel,
        out_shape=jax.ShapeDtypeStruct((2, 2 * depth, ny, nx), jnp.float32),
        in_specs=[anywhere] * 5 + [pl.BlockSpec(memory_space=pltpu.VMEM)] * 4,
        out_specs=anywhere,
        scratch_shapes=[
            pltpu.VMEM((2, 2 * depth, ny, nx), jnp.float32),
            pltpu.VMEM((2 * depth, ny, nx), jnp.float32),
            pltpu.SemaphoreType.DMA((2,)),
            pltpu.SemaphoreType.DMA((2,)),
            pltpu.SemaphoreType.DMA,
        ],
        compiler_params=pltpu.CompilerParams(vmem_limit_bytes=40 * 1024 * 1024),
        cost_estimate=pl.CostEstimate(
            flops=2 * points * 2 * 4 * nx, bytes_accessed=4 * points * 5, transcendentals=0
        ),
        name="near_field",
    )(owned[0], owned[1], visitor[0], visitor[1], order, *tables[:4])


def field_kernel(radix, first_call, rank_ref, *refs):
    refs = list(refs)

    def take(count):
        taken = refs[:count]
        del refs[:count]
        return taken

    own_hbm, vis_hbm = take(4), take(4)
    near_hbm, weights_hbm = take(2)
    tables = take(8)
    before_hbm = [] if first_call else take(2)
    held_hbm, sums_hbm = take(2), take(2)
    own_ref, vis_ref, real_ref, imag_ref, weights_ref, total_ref = take(6)
    own_sem, vis_sem, near_sem, weights_sem, before_sem, held_sem, sums_sem = refs
    nz, ny, _ = real_ref.shape
    depth = nz // 4
    rank = rank_ref[0]

    def base(slot):
        return lax.bitwise_xor(rank, slot) * depth

    own_in, vis_in, near_in, before_in, far_in = [], [], [], [], []
    half = depth // 2
    for s in range(2):
        here, part = pl.ds(base(s), depth), pl.ds(s * depth, depth)
        own_in.append(pltpu.make_async_copy(own_hbm[s], own_ref.at[:, here], own_sem.at[s, 0]))
        vis_in.append(pltpu.make_async_copy(vis_hbm[s], vis_ref.at[here], vis_sem.at[s, 0]))
        for i, ref in enumerate((real_ref, imag_ref)):
            near_in.append(
                pltpu.make_async_copy(near_hbm.at[i, part], ref.at[here], near_sem.at[s, i])
            )
        if not first_call:
            before_in.append(
                pltpu.make_async_copy(before_hbm[s], total_ref.at[:, part], before_sem.at[s])
            )
    for s in range(2, 4):
        for h in range(2):
            here, part = pl.ds(base(s) + h * half, half), pl.ds(h * half, half)
            far_in.append(
                [
                    pltpu.make_async_copy(
                        own_hbm[s].at[:, part], own_ref.at[:, here], own_sem.at[s, h]
                    ),
                    pltpu.make_async_copy(
                        vis_hbm[s].at[part], vis_ref.at[here], vis_sem.at[s, h]
                    ),
                ]
            )
    stripes = weights_sem.shape[0]
    stripe = ny // stripes
    weights_in = []
    for i in range(stripes):
        part = pl.ds(i * stripe, stripe)
        weights_in.append(
            pltpu.make_async_copy(
                weights_hbm.at[:, part], weights_ref.at[:, part], weights_sem.at[i]
            )
        )

    def start(copies):
        for copy in copies:
            copy.start()

    start(far_in[0])

    def loaded(index):
        return tables[index][...], tables[index + 1][...]

    def forward(z):
        here = pl.ds(z, 2)
        visitor = vis_ref[here]
        real, imag = transform_planes(
            own_ref[0, here] * visitor, own_ref[1, here] * visitor, loaded(0), loaded(2), False
        )
        real_ref[here] = real
        imag_ref[here] = imag

    def backward(z, kept):
        here = pl.ds(z, 2)
        real, imag = transform_planes(real_ref[here], imag_ref[here], loaded(6), loaded(4), True)
        visitor = vis_ref[here]
        vis_ref[here] = real * own_ref[0, here] + imag * own_ref[1, here]
        for i, part in enumerate((real, imag)):
            part = part * visitor
            if not first_call:
                part = part + total_ref[i, pl.ds(kept, 2)]
            total_ref[i, pl.ds(kept, 2)] = part

    def tile(index, carry):
        here = pl.ds(pl.multiple_of(8 * index, 8), 8)
        outer = nz // radix

        def load(z):
            return real_ref[z, here, :], imag_ref[z, here, :]

        def store(z, value):
            real_ref[z, here, :], imag_ref[z, here, :] = value

        for fine in range(radix):
            values = fourier([load(radix * n + fine) for n in range(outer)], -1.0)
            for k, value in enumerate(values):
                store(radix * k + fine, times(value, turn(fine * k, nz, -1.0)))
        for k in range(outer):
            values = fourier([load(radix * k + n) for n in range(radix)], -1.0)
            for n, (a, b) in enumerate(values):
                weight = weights_ref[radix * k + n, here, :]
                values[n] = (a * weight, b * weight)
            for n, value in enumerate(fourier(values, 1.0)):
                store(radix * k + n, value)
        for fine in range(radix):
            values = [times(load(radix * k + fine), turn(fine * k, nz, 1.0)) for k in range(outer)]
            for n, value in enumerate(fourier(values, 1.0)):
                store(radix * n + fine, value)
        return carry

    per_slot = depth // CHUNK

    def arrived(copies):
        for copy in copies:
            copy.wait()

    arrived(far_in[0])
    start(far_in[1] + near_in[:2])

    def forward_chunk(index, carry):
        per_half = per_slot // 2
        for h, later in (
            (1, far_in[2] + near_in[2:]),
            (2, far_in[3] + weights_in[:1]),
            (3, weights_in[1:]),
        ):

            @pl.when(index == h * per_half)
            def _():
                arrived(far_in[h])
                start(later)

        first = base(2 + index // per_slot) + index % per_slot * CHUNK
        for pair in range(CHUNK // 2):
            forward(first + 2 * pair)
        return carry

    lax.fori_loop(0, 2 * per_slot, forward_chunk, 0)
    arrived(near_in)

    def tile_and_wait(index, carry):
        for i in range(stripes):

            @pl.when(index == i * (stripe // 8))
            def _():
                arrived(weights_in[i : i + 1])
                if i == 1:
                    start(own_in[1::-1] + vis_in[1::-1] + before_in)

        return tile(index, carry)

    lax.fori_loop(0, ny // 8, tile_and_wait, 0)
    arrived(own_in + vis_in + before_in)

    def backward_chunk(index, carry):
        slot = 1 - index // per_slot
        first = index % per_slot * CHUNK
        for pair in range(CHUNK // 2):
            offset = first + 2 * pair
            backward(base(slot) + offset, slot * depth + offset)
        here = pl.ds(first, CHUNK)
        for s in range(2):

            @pl.when(slot == s)
            def _():
                pltpu.make_async_copy(
                    vis_ref.at[pl.ds(base(s) + first, CHUNK)], held_hbm[s].at[here], held_sem.at[s]
                ).start()
                pltpu.make_async_copy(
                    total_ref.at[:, pl.ds(s * depth + first, CHUNK)],
                    sums_hbm[s].at[:, here],
                    sums_sem.at[s],
                ).start()

        return carry

    lax.fori_loop(0, 2 * per_slot, backward_chunk, 0)
    for s in (1, 0):
        pltpu.make_async_copy(
            vis_ref.at[pl.ds(base(s), depth)], held_hbm[s], held_sem.at[s]
        ).wait()
        pltpu.make_async_copy(
            total_ref.at[:, pl.ds(s * depth, depth)], sums_hbm[s], sums_sem.at[s]
        ).wait()


def solve_field(rank, owned, visitor, near, weights, tables, before):
    depth, ny, nx = visitor[0].shape
    nz = 4 * depth
    first_call = before is None
    operands = list(owned) + list(visitor) + [near, weights] + list(tables)
    anywhere = pl.BlockSpec(memory_space=pl.ANY)
    in_specs = [pl.BlockSpec(memory_space=pltpu.SMEM)] + [anywhere] * 10
    in_specs += [pl.BlockSpec(memory_space=pltpu.VMEM)] * 8
    if not first_call:
        in_specs += [anywhere] * 2
        operands += list(before)
    shapes = [jax.ShapeDtypeStruct(v.shape, v.dtype) for v in visitor[:2]]
    shapes += [jax.ShapeDtypeStruct(v.shape, v.dtype) for v in owned[:2]]
    points = nz * ny * nx
    grid = pltpu.VMEM((nz, ny, nx), jnp.float32)
    results = pl.pallas_call(
        functools.partial(field_kernel, 8, first_call),
        out_shape=shapes,
        in_specs=in_specs,
        out_specs=[anywhere] * 4,
        scratch_shapes=[
            pltpu.VMEM((2, nz, ny, nx), jnp.float32),
            grid,
            grid,
            grid,
            grid,
            pltpu.VMEM((2, 2 * depth, ny, nx), jnp.float32),
            pltpu.SemaphoreType.DMA((4, 2)),
            pltpu.SemaphoreType.DMA((4, 2)),
            pltpu.SemaphoreType.DMA((2, 2)),
            pltpu.SemaphoreType.DMA((4,)),
            pltpu.SemaphoreType.DMA((2,)),
            pltpu.SemaphoreType.DMA((2,)),
            pltpu.SemaphoreType.DMA((2,)),
        ],
        compiler_params=pltpu.CompilerParams(vmem_limit_bytes=67043328),
        cost_estimate=pl.CostEstimate(
            flops=2 * points * 3 * 4 * nx, bytes_accessed=4 * points * 10, transcendentals=0
        ),
        name="solve_field",
    )(rank, *operands)
    return results[:2], results[2:]


def exchanged(block, bit):
    devices = range(lax.axis_size("grid"))
    return lax.ppermute(block, "grid", [(i, i ^ bit) for i in devices])


def picked(bands, first, count):
    return lax.dynamic_slice_in_dim(bands, first, count, 0)


def square_body(own_bands, travel_bands):
    rank = lax.axis_index("grid")
    core = rank % 2
    half_own = own_bands.shape[0] // 2
    count_vis = travel_bands.shape[0]
    depth, ny, nx = own_bands.shape[1:]
    nz = depth * lax.axis_size("grid")

    own_mine = picked(own_bands, core * half_own, half_own)
    own_far = exchanged(own_mine, 2)
    own_bands, travel_bands, _ = lax.optimization_barrier((own_bands, travel_bands, own_mine))
    own_side = exchanged(picked(own_bands, (1 - core) * half_own, half_own), 1)
    own_cross = exchanged(own_side, 2)
    owned = [own_mine, own_side, own_far, own_cross]

    visitors = []
    for j in range(count_vis):
        near = passed_along(travel_bands[j], "band", 1)
        far = exchanged(near, 2)
        side = exchanged(near, 1)
        cross = exchanged(far, 1)
        visitors.append([near, side, far, cross])

    radix = 8
    slot = jnp.arange(nz, dtype=jnp.int32)
    z_of_slot = slot // radix + (nz // radix) * (slot % radix)
    weights = (-FRACTION / (nz * ny * nx)) * coulomb(
        squared_wavenumber(z_of_slot, nz), wave_square(ny, 0, ny), wave_square(nx, 0, nx)
    )
    tables = []
    for length, inverse, left in (
        (nx, False, False),
        (ny, False, True),
        (ny, True, True),
        (nx, True, False),
    ):
        tables += halves(complex_matrix(length, inverse, left))
    rank_operand = rank.astype(jnp.int32).reshape(1)

    nears = []
    for j in range(count_vis):
        order = nears[-1] if nears else weights
        nears.append(near_field(owned, visitors[j], order, tables))

    sums = None
    returned = []
    for j in range(count_vis):
        held, sums = solve_field(rank_operand, owned, visitors[j], nears[j], weights, tables, sums)
        other = exchanged(held[1], 1)
        returned.append(passed_along(held[0] + other, "band", -1))

    own_other = exchanged(sums[1], 1)
    own_rows = jnp.zeros(own_bands.shape, own_bands.dtype)
    own_rows = lax.dynamic_update_slice_in_dim(own_rows, sums[0], core * half_own, 0)
    own_rows = lax.dynamic_update_slice_in_dim(own_rows, own_other, (1 - core) * half_own, 0)
    held_rows = jnp.zeros(travel_bands.shape, travel_bands.dtype)
    for j in range(count_vis):
        held_rows = lax.dynamic_update_slice_in_dim(held_rows, returned[j][None], j, 0)
    return own_rows, held_rows


def whole_body(own_bands, travel_bands):
    return square_body(own_bands, travel_bands)


def solution(mesh):
    spec = P("band", "grid", None, None)

    def placed(own_bands, travel_bands):
        group_own = own_bands.shape[0] // mesh.shape["band"]
        group_vis = travel_bands.shape[0] // mesh.shape["band"]
        square = mesh.shape["grid"] == 4 and group_own == 4 and group_vis % 2 == 0
        step = jax.shard_map(
            whole_body if square else body,
            mesh=mesh,
            in_specs=(spec, spec),
            out_specs=(spec, spec),
            check_vma=False,
        )
        return step(own_bands, travel_bands)

    return placed
```

```python
import functools
import math

import jax
import jax.numpy as jnp
import numpy as np
from jax import lax
from jax.experimental import pallas as pl
from jax.experimental.pallas import tpu as pltpu
from jax.sharding import PartitionSpec as P


FRACTION = 0.25
HIGHEST_PRECISION = lax.Precision.HIGHEST
CHUNK = 8
MESH = pl.DeviceIdType.MESH


def passed_along(block, axis, distance):
    devices = range(lax.axis_size(axis))
    route = [((i - distance) % len(devices), i) for i in devices]
    return lax.ppermute(block, axis, route)


def wave_square(points, first_row, length):
    position = first_row + jnp.arange(points, dtype=jnp.int32)
    return squared_wavenumber(position, length)


def squared_wavenumber(position, length):
    position = (position + length // 2) % length - length // 2
    wavenumber = 2.0 * math.pi / length * position.astype(jnp.float32)
    return wavenumber * wavenumber


def coulomb(square_z, square_y, square_x):
    squared = square_z[:, None, None] + square_y[None, :, None] + square_x[None, None, :]
    safe_square = jnp.where(squared > 0.0, squared, 1.0)
    return jnp.where(squared > 0.0, 4.0 * math.pi / safe_square, 0.0)


def fourier_table(length, inverse):
    position = jnp.arange(length, dtype=jnp.int32)
    phase_turns = position[:, None] * position[None, :] % length
    phase_angle = 2.0 * math.pi / length * phase_turns.astype(jnp.float32)
    cosine = jnp.cos(phase_angle)
    sine_part = jnp.sin(phase_angle)
    norm_factor = 1.0
    if inverse:
        sine_part = -sine_part
        norm_factor = 1.0 / length
    return norm_factor * jnp.stack(
        [jnp.stack([cosine, -sine_part]), jnp.stack([sine_part, cosine])]
    )


def solve_pairs(packed, kernel_slab, nz):
    ny, nx = packed.shape[3:]
    spectrum = jnp.einsum(
        "pczyx,cdxk->dpzyk", packed, fourier_table(nx, False), precision=HIGHEST_PRECISION
    )
    spectrum = jnp.einsum(
        "cpzyx,cdyk->dpzkx", spectrum, fourier_table(ny, False), precision=HIGHEST_PRECISION
    )
    forward_z = fourier_table(nz, False)
    inverse_z = fourier_table(nz, True)
    screened = (
        jnp.einsum(
            "cpzyx,cdzk->dpkyx",
            lax.all_to_all(spectrum, "grid", split_axis=3, concat_axis=2, tiled=True),
            forward_z,
            precision=HIGHEST_PRECISION,
        )
        * kernel_slab
    )
    screened = jnp.einsum("cpzyx,cdzk->dpkyx", screened, inverse_z, precision=HIGHEST_PRECISION)
    planes = lax.all_to_all(screened, "grid", split_axis=2, concat_axis=3, tiled=True)
    planes = jnp.einsum(
        "cpzyx,cdyk->dpzkx", planes, fourier_table(ny, True), precision=HIGHEST_PRECISION
    )
    return jnp.einsum(
        "cpzyx,cdxk->pdzyk", planes, fourier_table(nx, True), precision=HIGHEST_PRECISION
    )


def pair_terms(owned, visitors, kernel_slab, nz):
    count_vis = visitors.shape[0]
    count_own = owned.shape[0]
    density = owned[None] * visitors[:, None]
    packed = density.reshape((count_vis * count_own // 2, 2) + owned.shape[1:])
    potential = solve_pairs(packed, kernel_slab, nz).reshape(density.shape)
    own_part = jnp.sum(potential * visitors[:, None], axis=0)
    partner = jnp.sum(potential * owned[None], axis=1)
    return (own_part, partner)


def body(own_bands, travel_bands):
    depth, ny, nx = own_bands.shape[1:]
    nz = depth * lax.axis_size("grid")
    rows_local = ny // lax.axis_size("grid")
    kernel_slab = coulomb(
        wave_square(nz, 0, nz),
        wave_square(rows_local, lax.axis_index("grid") * rows_local, ny),
        wave_square(nx, 0, nx),
    )
    count_vis = travel_bands.shape[0]
    own_total = jnp.zeros_like(own_bands)
    returned = []
    for visit_index in range(count_vis):
        visitor = passed_along(travel_bands[visit_index : visit_index + 1], "band", 1)
        own_part, partner = pair_terms(own_bands, visitor, kernel_slab, nz)
        own_total = own_total + own_part
        returned.append(passed_along(partner, "band", -1))
    partner_total = jnp.concatenate(returned, axis=0)
    return (-FRACTION * own_total, -FRACTION * partner_total)


def halves(table):
    high = table.astype(jnp.bfloat16)
    return high, (table - high.astype(np.float32)).astype(jnp.bfloat16)


def complex_matrix(length, inverse, left):
    position = np.arange(length)
    angle = 2.0 * np.pi / length * (position[:, None] * position[None, :] % length)
    cosine, sine = np.cos(angle), np.sin(angle)
    if inverse:
        sine = -sine
    matrix = np.block([[cosine, -sine], [sine, cosine]])
    return (matrix.T if left else matrix).astype(np.float32)


def times(value, factor):
    (a, b), (c, d) = value, factor
    if abs(d) < 1e-12:
        return (a, b) if c > 0.5 else (-a, -b)
    if abs(c) < 1e-12:
        return (-b, a) if d > 0.0 else (b, -a)
    if abs(abs(c) - abs(d)) < 1e-12:
        size = abs(c)
        first = a if c > 0 else -a
        other = b if c > 0 else -b
        if (c > 0) == (d > 0):
            return size * (first - other), size * (first + other)
        return size * (first + other), size * (other - first)
    return a * c - b * d, a * d + b * c


def turn(numerator, length, sign):
    angle = 2.0 * math.pi * (numerator % length) / length
    return math.cos(angle), sign * math.sin(angle)


def fourier(values, sign):
    count = len(values)
    if count == 1:
        return values
    half = count // 2
    sums, differences = [], []
    for i in range(half):
        (a, b), (c, d) = values[i], values[i + half]
        sums.append((a + c, b + d))
        differences.append(times((a - c, b - d), turn(i, count, sign)))
    even = fourier(sums, sign)
    odd = fourier(differences, sign)
    return [pair for both in zip(even, odd) for pair in both]


def split(value):
    high = value.astype(jnp.bfloat16)
    return high, (value - high.astype(jnp.float32)).astype(jnp.bfloat16)


def dot(a, b):
    return jnp.dot(a, b, preferred_element_type=jnp.float32)


def product(left, right):
    (a, b), (c, d) = left, right
    return dot(a, c) + dot(b, c) + dot(a, d)


def transform_planes(real, imag, x_table, y_table, inverse):
    _, ny, nx = real.shape

    def along_x(real, imag):
        rows = jnp.concatenate([part.reshape(2 * ny, nx) for part in (real, imag)], axis=1)
        rows = product(split(rows), x_table)
        return [rows[:, i * nx : (i + 1) * nx].reshape(2, ny, nx) for i in (0, 1)]

    def along_y(real, imag):
        columns = jnp.concatenate(
            [jnp.concatenate([part[0], part[1]], axis=1) for part in (real, imag)], axis=0
        )
        columns = product(y_table, split(columns))
        return [
            jnp.stack([columns[i * ny : (i + 1) * ny, p * nx : (p + 1) * nx] for p in (0, 1)])
            for i in (0, 1)
        ]

    if inverse:
        return along_x(*along_y(real, imag))
    return along_y(*along_x(real, imag))


def near_kernel(own_0, own_1, vis_0, vis_1, order, x_high, x_low, y_high, y_low, out, *scratch):
    own_ref, vis_ref, own_sem, vis_sem, out_sem = scratch
    depth = vis_0.shape[0]
    own_hbm, vis_hbm = (own_0, own_1), (vis_0, vis_1)
    copies = []
    for s in range(2):
        part = pl.ds(s * depth, depth)
        copies.append(
            [
                pltpu.make_async_copy(own_hbm[s], own_ref.at[:, part], own_sem.at[s]),
                pltpu.make_async_copy(vis_hbm[s], vis_ref.at[part], vis_sem.at[s]),
            ]
        )
        for copy in copies[s]:
            copy.start()
    x_table = x_high[...], x_low[...]
    y_table = y_high[...], y_low[...]

    def slot(s, carry):
        part = pl.ds(s * depth, depth)
        pltpu.make_async_copy(own_0, own_ref.at[:, part], own_sem.at[s]).wait()
        pltpu.make_async_copy(vis_0, vis_ref.at[part], vis_sem.at[s]).wait()

        def chunk(index, carry):
            start = s * depth + index * CHUNK
            for pair in range(CHUNK // 2):
                here = pl.ds(start + 2 * pair, 2)
                visitor = vis_ref[here]
                real, imag = transform_planes(
                    own_ref[0, here] * visitor, own_ref[1, here] * visitor, x_table, y_table, False
                )
                own_ref[0, here] = real
                own_ref[1, here] = imag
            here = pl.ds(start, CHUNK)
            pltpu.make_async_copy(own_ref.at[:, here], out.at[:, here], out_sem).start()
            return carry

        return lax.fori_loop(0, depth // CHUNK, chunk, carry)

    lax.fori_loop(0, 2, slot, 0)
    pltpu.make_async_copy(own_ref, out, out_sem).wait()


def near_field(owned, visitor, order, tables):
    depth, ny, nx = visitor[0].shape
    anywhere = pl.BlockSpec(memory_space=pl.ANY)
    points = 2 * depth * ny * nx
    return pl.pallas_call(
        near_kernel,
        out_shape=jax.ShapeDtypeStruct((2, 2 * depth, ny, nx), jnp.float32),
        in_specs=[anywhere] * 5 + [pl.BlockSpec(memory_space=pltpu.VMEM)] * 4,
        out_specs=anywhere,
        scratch_shapes=[
            pltpu.VMEM((2, 2 * depth, ny, nx), jnp.float32),
            pltpu.VMEM((2 * depth, ny, nx), jnp.float32),
            pltpu.SemaphoreType.DMA((2,)),
            pltpu.SemaphoreType.DMA((2,)),
            pltpu.SemaphoreType.DMA,
        ],
        compiler_params=pltpu.CompilerParams(vmem_limit_bytes=40 * 1024 * 1024),
        cost_estimate=pl.CostEstimate(
            flops=2 * points * 2 * 4 * nx, bytes_accessed=4 * points * 5, transcendentals=0
        ),
        name="near_field",
    )(owned[0], owned[1], visitor[0], visitor[1], order, *tables[:4])


def field_kernel(radix, first_call, *refs):
    refs = list(refs)

    def take(count):
        taken = refs[:count]
        del refs[:count]
        return taken

    own_hbm, vis_hbm = take(4), take(4)
    near_hbm, weights_hbm = take(2)
    tables = take(8)
    before_hbm = [] if first_call else take(2)
    (held_hbm,), sums_hbm = take(1), take(2)
    own_ref, vis_ref, real_ref, imag_ref, weights_ref, total_ref, other_ref = take(7)
    own_sem, vis_sem, near_sem, weights_sem, before_sem, held_sem, sums_sem = take(7)
    send_sem, recv_sem = refs
    nz, ny, _ = real_ref.shape
    depth = nz // 4
    rank = lax.axis_index("grid")
    partner = {"grid": lax.bitwise_xor(rank, 1)}
    barrier = pltpu.get_barrier_semaphore()
    pl.semaphore_signal(barrier, inc=1, device_id=partner, device_id_type=MESH)

    def base(slot):
        return lax.bitwise_xor(rank, slot) * depth

    own_in, vis_in, near_in, before_in, far_in = [], [], [], [], []
    half = depth // 2
    for s in range(2):
        here, part = pl.ds(base(s), depth), pl.ds(s * depth, depth)
        own_in.append(pltpu.make_async_copy(own_hbm[s], own_ref.at[:, here], own_sem.at[s, 0]))
        vis_in.append(pltpu.make_async_copy(vis_hbm[s], vis_ref.at[here], vis_sem.at[s, 0]))
        for i, ref in enumerate((real_ref, imag_ref)):
            near_in.append(
                pltpu.make_async_copy(near_hbm.at[i, part], ref.at[here], near_sem.at[s, i])
            )
        if not first_call:
            before_in.append(
                pltpu.make_async_copy(before_hbm[s], total_ref.at[:, part], before_sem.at[s])
            )
    for s in range(2, 4):
        for h in range(2):
            here, part = pl.ds(base(s) + h * half, half), pl.ds(h * half, half)
            far_in.append(
                [
                    pltpu.make_async_copy(
                        own_hbm[s].at[:, part], own_ref.at[:, here], own_sem.at[s, h]
                    ),
                    pltpu.make_async_copy(
                        vis_hbm[s].at[part], vis_ref.at[here], vis_sem.at[s, h]
                    ),
                ]
            )
    stripes = weights_sem.shape[0]
    stripe = ny // stripes
    weights_in = []
    for i in range(stripes):
        part = pl.ds(i * stripe, stripe)
        weights_in.append(
            pltpu.make_async_copy(
                weights_hbm.at[:, part], weights_ref.at[:, part], weights_sem.at[i]
            )
        )

    def start(copies):
        for copy in copies:
            copy.start()

    start(far_in[0])

    def loaded(index):
        return tables[index][...], tables[index + 1][...]

    def forward(z):
        here = pl.ds(z, 2)
        visitor = vis_ref[here]
        real, imag = transform_planes(
            own_ref[0, here] * visitor, own_ref[1, here] * visitor, loaded(0), loaded(2), False
        )
        real_ref[here] = real
        imag_ref[here] = imag

    def backward(z, kept, other):
        here = pl.ds(z, 2)
        real, imag = transform_planes(real_ref[here], imag_ref[here], loaded(6), loaded(4), True)
        visitor = vis_ref[here]
        held = real * own_ref[0, here] + imag * own_ref[1, here]
        vis_ref[here] = held if other is None else held + other_ref[pl.ds(other, 2)]
        for i, part in enumerate((real, imag)):
            part = part * visitor
            if not first_call:
                part = part + total_ref[i, pl.ds(kept, 2)]
            total_ref[i, pl.ds(kept, 2)] = part

    def tile(index, carry):
        here = pl.ds(pl.multiple_of(8 * index, 8), 8)
        outer = nz // radix

        def load(z):
            return real_ref[z, here, :], imag_ref[z, here, :]

        def store(z, value):
            real_ref[z, here, :], imag_ref[z, here, :] = value

        for fine in range(radix):
            values = fourier([load(radix * n + fine) for n in range(outer)], -1.0)
            for k, value in enumerate(values):
                store(radix * k + fine, times(value, turn(fine * k, nz, -1.0)))
        for k in range(outer):
            values = fourier([load(radix * k + n) for n in range(radix)], -1.0)
            for n, (a, b) in enumerate(values):
                weight = weights_ref[radix * k + n, here, :]
                values[n] = (a * weight, b * weight)
            for n, value in enumerate(fourier(values, 1.0)):
                store(radix * k + n, value)
        for fine in range(radix):
            values = [times(load(radix * k + fine), turn(fine * k, nz, 1.0)) for k in range(outer)]
            for n, value in enumerate(fourier(values, 1.0)):
                store(radix * n + fine, value)
        return carry

    per_slot = depth // CHUNK

    def arrived(copies):
        for copy in copies:
            copy.wait()

    arrived(far_in[0])
    start(far_in[1] + near_in[:2])

    def forward_chunk(index, carry):
        per_half = per_slot // 2
        for h, later in (
            (1, far_in[2] + near_in[2:]),
            (2, far_in[3] + weights_in[:1]),
            (3, weights_in[1:]),
        ):

            @pl.when(index == h * per_half)
            def _():
                arrived(far_in[h])
                start(later)

        first = base(2 + index // per_slot) + index % per_slot * CHUNK
        for pair in range(CHUNK // 2):
            forward(first + 2 * pair)
        return carry

    lax.fori_loop(0, 2 * per_slot, forward_chunk, 0)
    arrived(near_in)

    def tile_and_wait(index, carry):
        for i in range(stripes):

            @pl.when(index == i * (stripe // 8))
            def _():
                arrived(weights_in[i : i + 1])
                if i == 1:
                    start(own_in[1::-1] + vis_in[1::-1] + before_in)

        return tile(index, carry)

    lax.fori_loop(0, ny // 8, tile_and_wait, 0)
    arrived(own_in + vis_in + before_in)

    pl.semaphore_wait(barrier, 1)

    def sent(index):
        part = pl.ds(index * CHUNK, CHUNK)
        return pltpu.make_async_remote_copy(
            src_ref=vis_ref.at[pl.ds(base(1) + index * CHUNK, CHUNK)],
            dst_ref=other_ref.at[part],
            send_sem=send_sem.at[index],
            recv_sem=recv_sem.at[index],
            device_id=partner,
            device_id_type=MESH,
        )

    def summed(slot, index):
        part = pl.ds(index * CHUNK, CHUNK)
        return pltpu.make_async_copy(
            total_ref.at[:, pl.ds(slot * depth + index * CHUNK, CHUNK)],
            sums_hbm[slot].at[:, part],
            sums_sem.at[slot],
        )

    def for_partner(index, carry):
        for pair in range(CHUNK // 2):
            offset = index * CHUNK + 2 * pair
            backward(base(1) + offset, depth + offset, None)
        sent(index).start()
        summed(1, index).start()
        return carry

    def for_self(index, carry):
        sent(index).wait_recv()
        for pair in range(CHUNK // 2):
            offset = index * CHUNK + 2 * pair
            backward(base(0) + offset, offset, offset)
        pltpu.make_async_copy(
            vis_ref.at[pl.ds(base(0) + index * CHUNK, CHUNK)],
            held_hbm.at[pl.ds(index * CHUNK, CHUNK)],
            held_sem,
        ).start()
        summed(0, index).start()
        return carry

    def left(index, carry):
        sent(index).wait_send()
        return carry

    lax.fori_loop(0, per_slot, for_partner, 0)
    lax.fori_loop(0, per_slot, for_self, 0)
    lax.fori_loop(0, per_slot, left, 0)
    pltpu.make_async_copy(vis_ref.at[pl.ds(base(0), depth)], held_hbm, held_sem).wait()
    for s in range(2):
        pltpu.make_async_copy(
            total_ref.at[:, pl.ds(s * depth, depth)], sums_hbm[s], sums_sem.at[s]
        ).wait()


def solve_field(owned, visitor, near, weights, tables, before):
    depth, ny, nx = visitor[0].shape
    nz = 4 * depth
    first_call = before is None
    operands = list(owned) + list(visitor) + [near, weights] + list(tables)
    anywhere = pl.BlockSpec(memory_space=pl.ANY)
    in_specs = [anywhere] * 10
    in_specs += [pl.BlockSpec(memory_space=pltpu.VMEM)] * 8
    if not first_call:
        in_specs += [anywhere] * 2
        operands += list(before)
    shapes = [jax.ShapeDtypeStruct(v.shape, v.dtype) for v in [visitor[0], *owned[:2]]]
    points = nz * ny * nx
    grid = pltpu.VMEM((nz, ny, nx), jnp.float32)
    results = pl.pallas_call(
        functools.partial(field_kernel, 8, first_call),
        out_shape=shapes,
        in_specs=in_specs,
        out_specs=[anywhere] * 3,
        scratch_shapes=[
            pltpu.VMEM((2, nz, ny, nx), jnp.float32),
            grid,
            grid,
            grid,
            grid,
            pltpu.VMEM((2, 2 * depth, ny, nx), jnp.float32),
            pltpu.VMEM((depth, ny, nx), jnp.float32),
            pltpu.SemaphoreType.DMA((4, 2)),
            pltpu.SemaphoreType.DMA((4, 2)),
            pltpu.SemaphoreType.DMA((2, 2)),
            pltpu.SemaphoreType.DMA((4,)),
            pltpu.SemaphoreType.DMA((2,)),
            pltpu.SemaphoreType.DMA,
            pltpu.SemaphoreType.DMA((2,)),
            pltpu.SemaphoreType.DMA((depth // CHUNK,)),
            pltpu.SemaphoreType.DMA((depth // CHUNK,)),
        ],
        compiler_params=pltpu.CompilerParams(
            vmem_limit_bytes=67043328,
            collective_id=0 if first_call else 1,
            has_side_effects=True,
        ),
        cost_estimate=pl.CostEstimate(
            flops=2 * points * 3 * 4 * nx, bytes_accessed=4 * points * 10, transcendentals=0
        ),
        name="solve_field",
    )(*operands)
    return results[0], results[1:]


def exchanged(block, bit):
    devices = range(lax.axis_size("grid"))
    return lax.ppermute(block, "grid", [(i, i ^ bit) for i in devices])


def picked(bands, first, count):
    return lax.dynamic_slice_in_dim(bands, first, count, 0)


def square_body(own_bands, travel_bands):
    rank = lax.axis_index("grid")
    core = rank % 2
    half_own = own_bands.shape[0] // 2
    count_vis = travel_bands.shape[0]
    depth, ny, nx = own_bands.shape[1:]
    nz = depth * lax.axis_size("grid")

    own_mine = picked(own_bands, core * half_own, half_own)
    own_far = exchanged(own_mine, 2)
    own_bands, travel_bands, _ = lax.optimization_barrier((own_bands, travel_bands, own_mine))
    own_side = exchanged(picked(own_bands, (1 - core) * half_own, half_own), 1)
    own_cross = exchanged(own_side, 2)
    owned = [own_mine, own_side, own_far, own_cross]

    visitors = []
    for j in range(count_vis):
        near = passed_along(travel_bands[j], "band", 1)
        far = exchanged(near, 2)
        side = exchanged(near, 1)
        cross = exchanged(far, 1)
        visitors.append([near, side, far, cross])

    radix = 8
    slot = jnp.arange(nz, dtype=jnp.int32)
    z_of_slot = slot // radix + (nz // radix) * (slot % radix)
    weights = (-FRACTION / (nz * ny * nx)) * coulomb(
        squared_wavenumber(z_of_slot, nz), wave_square(ny, 0, ny), wave_square(nx, 0, nx)
    )
    tables = []
    for length, inverse, left in (
        (nx, False, False),
        (ny, False, True),
        (ny, True, True),
        (nx, True, False),
    ):
        tables += halves(complex_matrix(length, inverse, left))

    nears = []
    for j in range(count_vis):
        order = nears[-1] if nears else weights
        nears.append(near_field(owned, visitors[j], order, tables))

    sums = None
    returned = []
    for j in range(count_vis):
        held, sums = solve_field(owned, visitors[j], nears[j], weights, tables, sums)
        returned.append(passed_along(held, "band", -1))

    own_other = exchanged(sums[1], 1)
    own_rows = jnp.zeros(own_bands.shape, own_bands.dtype)
    own_rows = lax.dynamic_update_slice_in_dim(own_rows, sums[0], core * half_own, 0)
    own_rows = lax.dynamic_update_slice_in_dim(own_rows, own_other, (1 - core) * half_own, 0)
    held_rows = jnp.zeros(travel_bands.shape, travel_bands.dtype)
    for j in range(count_vis):
        held_rows = lax.dynamic_update_slice_in_dim(held_rows, returned[j][None], j, 0)
    return own_rows, held_rows


def whole_body(own_bands, travel_bands):
    return square_body(own_bands, travel_bands)


def solution(mesh):
    spec = P("band", "grid", None, None)

    def placed(own_bands, travel_bands):
        group_own = own_bands.shape[0] // mesh.shape["band"]
        group_vis = travel_bands.shape[0] // mesh.shape["band"]
        square = mesh.shape["grid"] == 4 and group_own == 4 and group_vis % 2 == 0
        step = jax.shard_map(
            whole_body if square else body,
            mesh=mesh,
            in_specs=(spec, spec),
            out_specs=(spec, spec),
            check_vma=False,
        )
        return step(own_bands, travel_bands)

    return placed
```

```python
import functools
import math

import jax
import jax.numpy as jnp
import numpy as np
from jax import lax
from jax.experimental import pallas as pl
from jax.experimental.pallas import tpu as pltpu
from jax.sharding import PartitionSpec as P


FRACTION = 0.25
HIGHEST_PRECISION = lax.Precision.HIGHEST
CHUNK = 8
MESH = pl.DeviceIdType.MESH


def passed_along(block, axis, distance):
    devices = range(lax.axis_size(axis))
    route = [((i - distance) % len(devices), i) for i in devices]
    return lax.ppermute(block, axis, route)


def wave_square(points, first_row, length):
    position = first_row + jnp.arange(points, dtype=jnp.int32)
    return squared_wavenumber(position, length)


def squared_wavenumber(position, length):
    position = (position + length // 2) % length - length // 2
    wavenumber = 2.0 * math.pi / length * position.astype(jnp.float32)
    return wavenumber * wavenumber


def coulomb(square_z, square_y, square_x):
    squared = square_z[:, None, None] + square_y[None, :, None] + square_x[None, None, :]
    safe_square = jnp.where(squared > 0.0, squared, 1.0)
    return jnp.where(squared > 0.0, 4.0 * math.pi / safe_square, 0.0)


def fourier_table(length, inverse):
    position = jnp.arange(length, dtype=jnp.int32)
    phase_turns = position[:, None] * position[None, :] % length
    phase_angle = 2.0 * math.pi / length * phase_turns.astype(jnp.float32)
    cosine = jnp.cos(phase_angle)
    sine_part = jnp.sin(phase_angle)
    norm_factor = 1.0
    if inverse:
        sine_part = -sine_part
        norm_factor = 1.0 / length
    return norm_factor * jnp.stack(
        [jnp.stack([cosine, -sine_part]), jnp.stack([sine_part, cosine])]
    )


def solve_pairs(packed, kernel_slab, nz):
    ny, nx = packed.shape[3:]
    spectrum = jnp.einsum(
        "pczyx,cdxk->dpzyk", packed, fourier_table(nx, False), precision=HIGHEST_PRECISION
    )
    spectrum = jnp.einsum(
        "cpzyx,cdyk->dpzkx", spectrum, fourier_table(ny, False), precision=HIGHEST_PRECISION
    )
    forward_z = fourier_table(nz, False)
    inverse_z = fourier_table(nz, True)
    screened = (
        jnp.einsum(
            "cpzyx,cdzk->dpkyx",
            lax.all_to_all(spectrum, "grid", split_axis=3, concat_axis=2, tiled=True),
            forward_z,
            precision=HIGHEST_PRECISION,
        )
        * kernel_slab
    )
    screened = jnp.einsum("cpzyx,cdzk->dpkyx", screened, inverse_z, precision=HIGHEST_PRECISION)
    planes = lax.all_to_all(screened, "grid", split_axis=2, concat_axis=3, tiled=True)
    planes = jnp.einsum(
        "cpzyx,cdyk->dpzkx", planes, fourier_table(ny, True), precision=HIGHEST_PRECISION
    )
    return jnp.einsum(
        "cpzyx,cdxk->pdzyk", planes, fourier_table(nx, True), precision=HIGHEST_PRECISION
    )


def pair_terms(owned, visitors, kernel_slab, nz):
    count_vis = visitors.shape[0]
    count_own = owned.shape[0]
    density = owned[None] * visitors[:, None]
    packed = density.reshape((count_vis * count_own // 2, 2) + owned.shape[1:])
    potential = solve_pairs(packed, kernel_slab, nz).reshape(density.shape)
    own_part = jnp.sum(potential * visitors[:, None], axis=0)
    partner = jnp.sum(potential * owned[None], axis=1)
    return (own_part, partner)


def body(own_bands, travel_bands):
    depth, ny, nx = own_bands.shape[1:]
    nz = depth * lax.axis_size("grid")
    rows_local = ny // lax.axis_size("grid")
    kernel_slab = coulomb(
        wave_square(nz, 0, nz),
        wave_square(rows_local, lax.axis_index("grid") * rows_local, ny),
        wave_square(nx, 0, nx),
    )
    count_vis = travel_bands.shape[0]
    own_total = jnp.zeros_like(own_bands)
    returned = []
    for visit_index in range(count_vis):
        visitor = passed_along(travel_bands[visit_index : visit_index + 1], "band", 1)
        own_part, partner = pair_terms(own_bands, visitor, kernel_slab, nz)
        own_total = own_total + own_part
        returned.append(passed_along(partner, "band", -1))
    partner_total = jnp.concatenate(returned, axis=0)
    return (-FRACTION * own_total, -FRACTION * partner_total)


def halves(table):
    high = table.astype(jnp.bfloat16)
    return high, (table - high.astype(np.float32)).astype(jnp.bfloat16)


def complex_matrix(length, inverse, left):
    position = np.arange(length)
    angle = 2.0 * np.pi / length * (position[:, None] * position[None, :] % length)
    cosine, sine = np.cos(angle), np.sin(angle)
    if inverse:
        sine = -sine
    matrix = np.block([[cosine, -sine], [sine, cosine]])
    return (matrix.T if left else matrix).astype(np.float32)


def times(value, factor):
    (a, b), (c, d) = value, factor
    if abs(d) < 1e-12:
        return (a, b) if c > 0.5 else (-a, -b)
    if abs(c) < 1e-12:
        return (-b, a) if d > 0.0 else (b, -a)
    if abs(abs(c) - abs(d)) < 1e-12:
        size = abs(c)
        first = a if c > 0 else -a
        other = b if c > 0 else -b
        if (c > 0) == (d > 0):
            return size * (first - other), size * (first + other)
        return size * (first + other), size * (other - first)
    return a * c - b * d, a * d + b * c


def turn(numerator, length, sign):
    angle = 2.0 * math.pi * (numerator % length) / length
    return math.cos(angle), sign * math.sin(angle)


def fourier(values, sign):
    count = len(values)
    if count == 1:
        return values
    half = count // 2
    sums, differences = [], []
    for i in range(half):
        (a, b), (c, d) = values[i], values[i + half]
        sums.append((a + c, b + d))
        differences.append(times((a - c, b - d), turn(i, count, sign)))
    even = fourier(sums, sign)
    odd = fourier(differences, sign)
    return [pair for both in zip(even, odd) for pair in both]


def split(value):
    high = value.astype(jnp.bfloat16)
    return high, (value - high.astype(jnp.float32)).astype(jnp.bfloat16)


def dot(a, b):
    return jnp.dot(a, b, preferred_element_type=jnp.float32)


def product(left, right):
    (a, b), (c, d) = left, right
    return dot(a, c) + dot(b, c) + dot(a, d)


def transform_planes(real, imag, x_table, y_table, inverse):
    _, ny, nx = real.shape

    def along_x(real, imag):
        rows = jnp.concatenate([part.reshape(2 * ny, nx) for part in (real, imag)], axis=1)
        rows = product(split(rows), x_table)
        return [rows[:, i * nx : (i + 1) * nx].reshape(2, ny, nx) for i in (0, 1)]

    def along_y(real, imag):
        columns = jnp.concatenate(
            [jnp.concatenate([part[0], part[1]], axis=1) for part in (real, imag)], axis=0
        )
        columns = product(y_table, split(columns))
        return [
            jnp.stack([columns[i * ny : (i + 1) * ny, p * nx : (p + 1) * nx] for p in (0, 1)])
            for i in (0, 1)
        ]

    if inverse:
        return along_x(*along_y(real, imag))
    return along_y(*along_x(real, imag))


def near_kernel(own_0, own_1, vis_0, vis_1, order, x_high, x_low, y_high, y_low, out, *scratch):
    own_ref, vis_ref, own_sem, vis_sem, out_sem = scratch
    depth = vis_0.shape[0]
    own_hbm, vis_hbm = (own_0, own_1), (vis_0, vis_1)
    copies = []
    for s in range(2):
        part = pl.ds(s * depth, depth)
        copies.append(
            [
                pltpu.make_async_copy(own_hbm[s], own_ref.at[:, part], own_sem.at[s]),
                pltpu.make_async_copy(vis_hbm[s], vis_ref.at[part], vis_sem.at[s]),
            ]
        )
        for copy in copies[s]:
            copy.start()
    x_table = x_high[...], x_low[...]
    y_table = y_high[...], y_low[...]

    def slot(s, carry):
        part = pl.ds(s * depth, depth)
        pltpu.make_async_copy(own_0, own_ref.at[:, part], own_sem.at[s]).wait()
        pltpu.make_async_copy(vis_0, vis_ref.at[part], vis_sem.at[s]).wait()

        def chunk(index, carry):
            start = s * depth + index * CHUNK
            for pair in range(CHUNK // 2):
                here = pl.ds(start + 2 * pair, 2)
                visitor = vis_ref[here]
                real, imag = transform_planes(
                    own_ref[0, here] * visitor, own_ref[1, here] * visitor, x_table, y_table, False
                )
                own_ref[0, here] = real
                own_ref[1, here] = imag
            here = pl.ds(start, CHUNK)
            pltpu.make_async_copy(own_ref.at[:, here], out.at[:, here], out_sem).start()
            return carry

        return lax.fori_loop(0, depth // CHUNK, chunk, carry)

    lax.fori_loop(0, 2, slot, 0)
    pltpu.make_async_copy(own_ref, out, out_sem).wait()


def near_field(owned, visitor, order, tables):
    depth, ny, nx = visitor[0].shape
    anywhere = pl.BlockSpec(memory_space=pl.ANY)
    points = 2 * depth * ny * nx
    return pl.pallas_call(
        near_kernel,
        out_shape=jax.ShapeDtypeStruct((2, 2 * depth, ny, nx), jnp.float32),
        in_specs=[anywhere] * 5 + [pl.BlockSpec(memory_space=pltpu.VMEM)] * 4,
        out_specs=anywhere,
        scratch_shapes=[
            pltpu.VMEM((2, 2 * depth, ny, nx), jnp.float32),
            pltpu.VMEM((2 * depth, ny, nx), jnp.float32),
            pltpu.SemaphoreType.DMA((2,)),
            pltpu.SemaphoreType.DMA((2,)),
            pltpu.SemaphoreType.DMA,
        ],
        compiler_params=pltpu.CompilerParams(vmem_limit_bytes=40 * 1024 * 1024),
        cost_estimate=pl.CostEstimate(
            flops=2 * points * 2 * 4 * nx, bytes_accessed=4 * points * 5, transcendentals=0
        ),
        name="near_field",
    )(owned[0], owned[1], visitor[0], visitor[1], order, *tables[:4])


def field_kernel(radix, first_call, *refs):
    refs = list(refs)

    def take(count):
        taken = refs[:count]
        del refs[:count]
        return taken

    own_hbm, vis_hbm = take(4), take(3)
    near_hbm, weights_hbm = take(2)
    tables = take(8)
    before_hbm = [] if first_call else take(2)
    (held_hbm,), sums_hbm = take(1), take(2)
    own_ref, vis_ref, real_ref, imag_ref, weights_ref, total_ref, other_ref = take(7)
    own_sem, vis_sem, near_sem, weights_sem, before_sem, held_sem, sums_sem = take(7)
    send_sem, recv_sem, cross_sem, crossed_sem = refs
    nz, ny, _ = real_ref.shape
    depth = nz // 4
    rank = lax.axis_index("grid")
    partner = {"grid": lax.bitwise_xor(rank, 1)}
    barrier = pltpu.get_barrier_semaphore()
    pl.semaphore_signal(barrier, inc=1, device_id=partner, device_id_type=MESH)

    def base(slot):
        return lax.bitwise_xor(rank, slot) * depth

    own_in, vis_in, near_in, before_in, far_in = [], [], [], [], []
    half = depth // 2
    for s in range(2):
        here, part = pl.ds(base(s), depth), pl.ds(s * depth, depth)
        own_in.append(pltpu.make_async_copy(own_hbm[s], own_ref.at[:, here], own_sem.at[s, 0]))
        vis_in.append(pltpu.make_async_copy(vis_hbm[s], vis_ref.at[here], vis_sem.at[s, 0]))
        for i, ref in enumerate((real_ref, imag_ref)):
            near_in.append(
                pltpu.make_async_copy(near_hbm.at[i, part], ref.at[here], near_sem.at[s, i])
            )
        if not first_call:
            before_in.append(
                pltpu.make_async_copy(before_hbm[s], total_ref.at[:, part], before_sem.at[s])
            )
    for s in range(2, 4):
        for h in range(2):
            here, part = pl.ds(base(s) + h * half, half), pl.ds(h * half, half)
            far_in.append(
                [
                    pltpu.make_async_copy(
                        own_hbm[s].at[:, part], own_ref.at[:, here], own_sem.at[s, h]
                    )
                ]
            )
            if s == 2:
                far_in[-1].append(
                    pltpu.make_async_copy(
                        vis_hbm[s].at[part], vis_ref.at[here], vis_sem.at[s, h]
                    )
                )
    stripes = weights_sem.shape[0]
    stripe = ny // stripes
    weights_in = []
    for i in range(stripes):
        part = pl.ds(i * stripe, stripe)
        weights_in.append(
            pltpu.make_async_copy(
                weights_hbm.at[:, part], weights_ref.at[:, part], weights_sem.at[i]
            )
        )

    def start(copies):
        for copy in copies:
            copy.start()

    def crossing(h):
        return pltpu.make_async_remote_copy(
            src_ref=vis_hbm[2].at[pl.ds(h * half, half)],
            dst_ref=vis_ref.at[pl.ds(base(2) + h * half, half)],
            send_sem=cross_sem.at[h],
            recv_sem=crossed_sem.at[h],
            device_id=partner,
            device_id_type=MESH,
        )

    start(far_in[0])
    pl.semaphore_wait(barrier, 1)
    start([crossing(0), crossing(1)])

    def loaded(index):
        return tables[index][...], tables[index + 1][...]

    def forward(z):
        here = pl.ds(z, 2)
        visitor = vis_ref[here]
        real, imag = transform_planes(
            own_ref[0, here] * visitor, own_ref[1, here] * visitor, loaded(0), loaded(2), False
        )
        real_ref[here] = real
        imag_ref[here] = imag

    def backward(z, kept, other):
        here = pl.ds(z, 2)
        real, imag = transform_planes(real_ref[here], imag_ref[here], loaded(6), loaded(4), True)
        visitor = vis_ref[here]
        held = real * own_ref[0, here] + imag * own_ref[1, here]
        vis_ref[here] = held if other is None else held + other_ref[pl.ds(other, 2)]
        for i, part in enumerate((real, imag)):
            part = part * visitor
            if not first_call:
                part = part + total_ref[i, pl.ds(kept, 2)]
            total_ref[i, pl.ds(kept, 2)] = part

    def tile(index, carry):
        here = pl.ds(pl.multiple_of(8 * index, 8), 8)
        outer = nz // radix

        def load(z):
            return real_ref[z, here, :], imag_ref[z, here, :]

        def store(z, value):
            real_ref[z, here, :], imag_ref[z, here, :] = value

        for fine in range(radix):
            values = fourier([load(radix * n + fine) for n in range(outer)], -1.0)
            for k, value in enumerate(values):
                store(radix * k + fine, times(value, turn(fine * k, nz, -1.0)))
        for k in range(outer):
            values = fourier([load(radix * k + n) for n in range(radix)], -1.0)
            for n, (a, b) in enumerate(values):
                weight = weights_ref[radix * k + n, here, :]
                values[n] = (a * weight, b * weight)
            for n, value in enumerate(fourier(values, 1.0)):
                store(radix * k + n, value)
        for fine in range(radix):
            values = [times(load(radix * k + fine), turn(fine * k, nz, 1.0)) for k in range(outer)]
            for n, value in enumerate(fourier(values, 1.0)):
                store(radix * n + fine, value)
        return carry

    per_slot = depth // CHUNK

    def arrived(copies):
        for copy in copies:
            copy.wait()

    arrived(far_in[0])
    start(far_in[1] + near_in[:2])

    def forward_chunk(index, carry):
        per_half = per_slot // 2
        for h, later in (
            (1, far_in[2] + near_in[2:]),
            (2, far_in[3] + weights_in[:1]),
            (3, weights_in[1:]),
        ):

            @pl.when(index == h * per_half)
            def _():
                arrived(far_in[h])
                if h >= 2:
                    crossing(h - 2).wait_recv()
                start(later)

        first = base(2 + index // per_slot) + index % per_slot * CHUNK
        for pair in range(CHUNK // 2):
            forward(first + 2 * pair)
        return carry

    lax.fori_loop(0, 2 * per_slot, forward_chunk, 0)
    arrived(near_in)

    def tile_and_wait(index, carry):
        for i in range(stripes):

            @pl.when(index == i * (stripe // 8))
            def _():
                arrived(weights_in[i : i + 1])
                if i == 1:
                    start(own_in[1::-1] + vis_in[1::-1] + before_in)

        return tile(index, carry)

    lax.fori_loop(0, ny // 8, tile_and_wait, 0)
    arrived(own_in + vis_in + before_in)

    def sent(index):
        part = pl.ds(index * CHUNK, CHUNK)
        return pltpu.make_async_remote_copy(
            src_ref=vis_ref.at[pl.ds(base(1) + index * CHUNK, CHUNK)],
            dst_ref=other_ref.at[part],
            send_sem=send_sem.at[index],
            recv_sem=recv_sem.at[index],
            device_id=partner,
            device_id_type=MESH,
        )

    def summed(slot, index):
        part = pl.ds(index * CHUNK, CHUNK)
        return pltpu.make_async_copy(
            total_ref.at[:, pl.ds(slot * depth + index * CHUNK, CHUNK)],
            sums_hbm[slot].at[:, part],
            sums_sem.at[slot],
        )

    def for_partner(index, carry):
        for pair in range(CHUNK // 2):
            offset = index * CHUNK + 2 * pair
            backward(base(1) + offset, depth + offset, None)
        sent(index).start()
        summed(1, index).start()
        return carry

    def for_self(index, carry):
        sent(index).wait_recv()
        for pair in range(CHUNK // 2):
            offset = index * CHUNK + 2 * pair
            backward(base(0) + offset, offset, offset)
        pltpu.make_async_copy(
            vis_ref.at[pl.ds(base(0) + index * CHUNK, CHUNK)],
            held_hbm.at[pl.ds(index * CHUNK, CHUNK)],
            held_sem,
        ).start()
        summed(0, index).start()
        return carry

    def left(index, carry):
        sent(index).wait_send()
        return carry

    lax.fori_loop(0, per_slot, for_partner, 0)
    lax.fori_loop(0, per_slot, for_self, 0)
    lax.fori_loop(0, per_slot, left, 0)
    for h in range(2):
        crossing(h).wait_send()
    pltpu.make_async_copy(vis_ref.at[pl.ds(base(0), depth)], held_hbm, held_sem).wait()
    for s in range(2):
        pltpu.make_async_copy(
            total_ref.at[:, pl.ds(s * depth, depth)], sums_hbm[s], sums_sem.at[s]
        ).wait()


def solve_field(owned, visitor, near, weights, tables, before):
    depth, ny, nx = visitor[0].shape
    nz = 4 * depth
    first_call = before is None
    operands = list(owned) + list(visitor) + [near, weights] + list(tables)
    anywhere = pl.BlockSpec(memory_space=pl.ANY)
    in_specs = [anywhere] * 9
    in_specs += [pl.BlockSpec(memory_space=pltpu.VMEM)] * 8
    if not first_call:
        in_specs += [anywhere] * 2
        operands += list(before)
    shapes = [jax.ShapeDtypeStruct(v.shape, v.dtype) for v in [visitor[0], *owned[:2]]]
    points = nz * ny * nx
    grid = pltpu.VMEM((nz, ny, nx), jnp.float32)
    results = pl.pallas_call(
        functools.partial(field_kernel, 8, first_call),
        out_shape=shapes,
        in_specs=in_specs,
        out_specs=[anywhere] * 3,
        scratch_shapes=[
            pltpu.VMEM((2, nz, ny, nx), jnp.float32),
            grid,
            grid,
            grid,
            grid,
            pltpu.VMEM((2, 2 * depth, ny, nx), jnp.float32),
            pltpu.VMEM((depth, ny, nx), jnp.float32),
            pltpu.SemaphoreType.DMA((4, 2)),
            pltpu.SemaphoreType.DMA((4, 2)),
            pltpu.SemaphoreType.DMA((2, 2)),
            pltpu.SemaphoreType.DMA((4,)),
            pltpu.SemaphoreType.DMA((2,)),
            pltpu.SemaphoreType.DMA,
            pltpu.SemaphoreType.DMA((2,)),
            pltpu.SemaphoreType.DMA((depth // CHUNK,)),
            pltpu.SemaphoreType.DMA((depth // CHUNK,)),
            pltpu.SemaphoreType.DMA((2,)),
            pltpu.SemaphoreType.DMA((2,)),
        ],
        compiler_params=pltpu.CompilerParams(
            vmem_limit_bytes=67043328,
            collective_id=0 if first_call else 1,
            has_side_effects=True,
        ),
        cost_estimate=pl.CostEstimate(
            flops=2 * points * 3 * 4 * nx, bytes_accessed=4 * points * 10, transcendentals=0
        ),
        name="solve_field",
    )(*operands)
    return results[0], results[1:]


def exchanged(block, bit):
    devices = range(lax.axis_size("grid"))
    return lax.ppermute(block, "grid", [(i, i ^ bit) for i in devices])


def picked(bands, first, count):
    return lax.dynamic_slice_in_dim(bands, first, count, 0)


def square_body(own_bands, travel_bands):
    rank = lax.axis_index("grid")
    core = rank % 2
    half_own = own_bands.shape[0] // 2
    count_vis = travel_bands.shape[0]
    depth, ny, nx = own_bands.shape[1:]
    nz = depth * lax.axis_size("grid")

    own_mine = picked(own_bands, core * half_own, half_own)
    own_far = exchanged(own_mine, 2)
    own_bands, travel_bands, _ = lax.optimization_barrier((own_bands, travel_bands, own_mine))
    own_side = exchanged(picked(own_bands, (1 - core) * half_own, half_own), 1)
    own_cross = exchanged(own_side, 2)
    owned = [own_mine, own_side, own_far, own_cross]

    visitors = []
    for j in range(count_vis):
        near = passed_along(travel_bands[j], "band", 1)
        far = exchanged(near, 2)
        side = exchanged(near, 1)
        visitors.append([near, side, far])

    radix = 8
    slot = jnp.arange(nz, dtype=jnp.int32)
    z_of_slot = slot // radix + (nz // radix) * (slot % radix)
    weights = (-FRACTION / (nz * ny * nx)) * coulomb(
        squared_wavenumber(z_of_slot, nz), wave_square(ny, 0, ny), wave_square(nx, 0, nx)
    )
    tables = []
    for length, inverse, left in (
        (nx, False, False),
        (ny, False, True),
        (ny, True, True),
        (nx, True, False),
    ):
        tables += halves(complex_matrix(length, inverse, left))

    nears = []
    for j in range(count_vis):
        order = nears[-1] if nears else weights
        nears.append(near_field(owned, visitors[j], order, tables))

    sums = None
    returned = []
    for j in range(count_vis):
        held, sums = solve_field(owned, visitors[j], nears[j], weights, tables, sums)
        returned.append(passed_along(held, "band", -1))

    own_other = exchanged(sums[1], 1)
    own_rows = jnp.zeros(own_bands.shape, own_bands.dtype)
    own_rows = lax.dynamic_update_slice_in_dim(own_rows, sums[0], core * half_own, 0)
    own_rows = lax.dynamic_update_slice_in_dim(own_rows, own_other, (1 - core) * half_own, 0)
    held_rows = jnp.zeros(travel_bands.shape, travel_bands.dtype)
    for j in range(count_vis):
        held_rows = lax.dynamic_update_slice_in_dim(held_rows, returned[j][None], j, 0)
    return own_rows, held_rows


def whole_body(own_bands, travel_bands):
    return square_body(own_bands, travel_bands)


def solution(mesh):
    spec = P("band", "grid", None, None)

    def placed(own_bands, travel_bands):
        group_own = own_bands.shape[0] // mesh.shape["band"]
        group_vis = travel_bands.shape[0] // mesh.shape["band"]
        square = mesh.shape["grid"] == 4 and group_own == 4 and group_vis % 2 == 0
        step = jax.shard_map(
            whole_body if square else body,
            mesh=mesh,
            in_specs=(spec, spec),
            out_specs=(spec, spec),
            check_vma=False,
        )
        return step(own_bands, travel_bands)

    return placed
```

```python
import functools
import math

import jax
import jax.numpy as jnp
import numpy as np
from jax import lax
from jax.experimental import pallas as pl
from jax.experimental.pallas import tpu as pltpu
from jax.sharding import PartitionSpec as P


FRACTION = 0.25
HIGHEST_PRECISION = lax.Precision.HIGHEST
CHUNK = 8
MESH = pl.DeviceIdType.MESH


def passed_along(block, axis, distance):
    devices = range(lax.axis_size(axis))
    route = [((i - distance) % len(devices), i) for i in devices]
    return lax.ppermute(block, axis, route)


def wave_square(points, first_row, length):
    position = first_row + jnp.arange(points, dtype=jnp.int32)
    return squared_wavenumber(position, length)


def squared_wavenumber(position, length):
    position = (position + length // 2) % length - length // 2
    wavenumber = 2.0 * math.pi / length * position.astype(jnp.float32)
    return wavenumber * wavenumber


def coulomb(square_z, square_y, square_x):
    squared = square_z[:, None, None] + square_y[None, :, None] + square_x[None, None, :]
    safe_square = jnp.where(squared > 0.0, squared, 1.0)
    return jnp.where(squared > 0.0, 4.0 * math.pi / safe_square, 0.0)


def fourier_table(length, inverse):
    position = jnp.arange(length, dtype=jnp.int32)
    phase_turns = position[:, None] * position[None, :] % length
    phase_angle = 2.0 * math.pi / length * phase_turns.astype(jnp.float32)
    cosine = jnp.cos(phase_angle)
    sine_part = jnp.sin(phase_angle)
    norm_factor = 1.0
    if inverse:
        sine_part = -sine_part
        norm_factor = 1.0 / length
    return norm_factor * jnp.stack(
        [jnp.stack([cosine, -sine_part]), jnp.stack([sine_part, cosine])]
    )


def solve_pairs(packed, kernel_slab, nz):
    ny, nx = packed.shape[3:]
    spectrum = jnp.einsum(
        "pczyx,cdxk->dpzyk", packed, fourier_table(nx, False), precision=HIGHEST_PRECISION
    )
    spectrum = jnp.einsum(
        "cpzyx,cdyk->dpzkx", spectrum, fourier_table(ny, False), precision=HIGHEST_PRECISION
    )
    forward_z = fourier_table(nz, False)
    inverse_z = fourier_table(nz, True)
    screened = (
        jnp.einsum(
            "cpzyx,cdzk->dpkyx",
            lax.all_to_all(spectrum, "grid", split_axis=3, concat_axis=2, tiled=True),
            forward_z,
            precision=HIGHEST_PRECISION,
        )
        * kernel_slab
    )
    screened = jnp.einsum("cpzyx,cdzk->dpkyx", screened, inverse_z, precision=HIGHEST_PRECISION)
    planes = lax.all_to_all(screened, "grid", split_axis=2, concat_axis=3, tiled=True)
    planes = jnp.einsum(
        "cpzyx,cdyk->dpzkx", planes, fourier_table(ny, True), precision=HIGHEST_PRECISION
    )
    return jnp.einsum(
        "cpzyx,cdxk->pdzyk", planes, fourier_table(nx, True), precision=HIGHEST_PRECISION
    )


def pair_terms(owned, visitors, kernel_slab, nz):
    count_vis = visitors.shape[0]
    count_own = owned.shape[0]
    density = owned[None] * visitors[:, None]
    packed = density.reshape((count_vis * count_own // 2, 2) + owned.shape[1:])
    potential = solve_pairs(packed, kernel_slab, nz).reshape(density.shape)
    own_part = jnp.sum(potential * visitors[:, None], axis=0)
    partner = jnp.sum(potential * owned[None], axis=1)
    return (own_part, partner)


def body(own_bands, travel_bands):
    depth, ny, nx = own_bands.shape[1:]
    nz = depth * lax.axis_size("grid")
    rows_local = ny // lax.axis_size("grid")
    kernel_slab = coulomb(
        wave_square(nz, 0, nz),
        wave_square(rows_local, lax.axis_index("grid") * rows_local, ny),
        wave_square(nx, 0, nx),
    )
    count_vis = travel_bands.shape[0]
    own_total = jnp.zeros_like(own_bands)
    returned = []
    for visit_index in range(count_vis):
        visitor = passed_along(travel_bands[visit_index : visit_index + 1], "band", 1)
        own_part, partner = pair_terms(own_bands, visitor, kernel_slab, nz)
        own_total = own_total + own_part
        returned.append(passed_along(partner, "band", -1))
    partner_total = jnp.concatenate(returned, axis=0)
    return (-FRACTION * own_total, -FRACTION * partner_total)


def halves(table):
    high = table.astype(jnp.bfloat16)
    return high, (table - high.astype(np.float32)).astype(jnp.bfloat16)


def complex_matrix(length, inverse, left):
    position = np.arange(length)
    angle = 2.0 * np.pi / length * (position[:, None] * position[None, :] % length)
    cosine, sine = np.cos(angle), np.sin(angle)
    if inverse:
        sine = -sine
    matrix = np.block([[cosine, -sine], [sine, cosine]])
    return (matrix.T if left else matrix).astype(np.float32)


def times(value, factor):
    (a, b), (c, d) = value, factor
    if abs(d) < 1e-12:
        return (a, b) if c > 0.5 else (-a, -b)
    if abs(c) < 1e-12:
        return (-b, a) if d > 0.0 else (b, -a)
    if abs(abs(c) - abs(d)) < 1e-12:
        size = abs(c)
        first = a if c > 0 else -a
        other = b if c > 0 else -b
        if (c > 0) == (d > 0):
            return size * (first - other), size * (first + other)
        return size * (first + other), size * (other - first)
    return a * c - b * d, a * d + b * c


def turn(numerator, length, sign):
    angle = 2.0 * math.pi * (numerator % length) / length
    return math.cos(angle), sign * math.sin(angle)


def fourier(values, sign):
    count = len(values)
    if count == 1:
        return values
    half = count // 2
    sums, differences = [], []
    for i in range(half):
        (a, b), (c, d) = values[i], values[i + half]
        sums.append((a + c, b + d))
        differences.append(times((a - c, b - d), turn(i, count, sign)))
    even = fourier(sums, sign)
    odd = fourier(differences, sign)
    return [pair for both in zip(even, odd) for pair in both]


def split(value):
    high = value.astype(jnp.bfloat16)
    return high, (value - high.astype(jnp.float32)).astype(jnp.bfloat16)


def dot(a, b):
    return jnp.dot(a, b, preferred_element_type=jnp.float32)


def product(left, right):
    (a, b), (c, d) = left, right
    return dot(a, c) + dot(b, c) + dot(a, d)


def transform_planes(real, imag, x_table, y_table, inverse):
    _, ny, nx = real.shape

    def along_x(real, imag):
        rows = jnp.concatenate([part.reshape(2 * ny, nx) for part in (real, imag)], axis=1)
        rows = product(split(rows), x_table)
        return [rows[:, i * nx : (i + 1) * nx].reshape(2, ny, nx) for i in (0, 1)]

    def along_y(real, imag):
        columns = jnp.concatenate(
            [jnp.concatenate([part[0], part[1]], axis=1) for part in (real, imag)], axis=0
        )
        columns = product(y_table, split(columns))
        return [
            jnp.stack([columns[i * ny : (i + 1) * ny, p * nx : (p + 1) * nx] for p in (0, 1)])
            for i in (0, 1)
        ]

    if inverse:
        return along_x(*along_y(real, imag))
    return along_y(*along_x(real, imag))


def near_kernel(own_0, own_1, vis_0, vis_1, order, x_high, x_low, y_high, y_low, out, *scratch):
    own_ref, vis_ref, own_sem, vis_sem, out_sem = scratch
    depth = vis_0.shape[0]
    own_hbm, vis_hbm = (own_0, own_1), (vis_0, vis_1)
    copies = []
    for s in range(2):
        part = pl.ds(s * depth, depth)
        copies.append(
            [
                pltpu.make_async_copy(own_hbm[s], own_ref.at[:, part], own_sem.at[s]),
                pltpu.make_async_copy(vis_hbm[s], vis_ref.at[part], vis_sem.at[s]),
            ]
        )
        for copy in copies[s]:
            copy.start()
    x_table = x_high[...], x_low[...]
    y_table = y_high[...], y_low[...]

    def slot(s, carry):
        part = pl.ds(s * depth, depth)
        pltpu.make_async_copy(own_0, own_ref.at[:, part], own_sem.at[s]).wait()
        pltpu.make_async_copy(vis_0, vis_ref.at[part], vis_sem.at[s]).wait()

        def chunk(index, carry):
            start = s * depth + index * CHUNK
            for pair in range(CHUNK // 2):
                here = pl.ds(start + 2 * pair, 2)
                visitor = vis_ref[here]
                real, imag = transform_planes(
                    own_ref[0, here] * visitor, own_ref[1, here] * visitor, x_table, y_table, False
                )
                own_ref[0, here] = real
                own_ref[1, here] = imag
            here = pl.ds(start, CHUNK)
            pltpu.make_async_copy(own_ref.at[:, here], out.at[:, here], out_sem).start()
            return carry

        return lax.fori_loop(0, depth // CHUNK, chunk, carry)

    lax.fori_loop(0, 2, slot, 0)
    pltpu.make_async_copy(own_ref, out, out_sem).wait()


def near_field(owned, visitor, order, tables):
    depth, ny, nx = visitor[0].shape
    anywhere = pl.BlockSpec(memory_space=pl.ANY)
    points = 2 * depth * ny * nx
    return pl.pallas_call(
        near_kernel,
        out_shape=jax.ShapeDtypeStruct((2, 2 * depth, ny, nx), jnp.float32),
        in_specs=[anywhere] * 5 + [pl.BlockSpec(memory_space=pltpu.VMEM)] * 4,
        out_specs=anywhere,
        scratch_shapes=[
            pltpu.VMEM((2, 2 * depth, ny, nx), jnp.float32),
            pltpu.VMEM((2 * depth, ny, nx), jnp.float32),
            pltpu.SemaphoreType.DMA((2,)),
            pltpu.SemaphoreType.DMA((2,)),
            pltpu.SemaphoreType.DMA,
        ],
        compiler_params=pltpu.CompilerParams(vmem_limit_bytes=40 * 1024 * 1024),
        cost_estimate=pl.CostEstimate(
            flops=2 * points * 2 * 4 * nx, bytes_accessed=4 * points * 5, transcendentals=0
        ),
        name="near_field",
    )(owned[0], owned[1], visitor[0], visitor[1], order, *tables[:4])


def field_kernel(radix, first_call, *refs):
    refs = list(refs)

    def take(count):
        taken = refs[:count]
        del refs[:count]
        return taken

    own_hbm, vis_hbm = take(4), take(3)
    near_hbm, weights_hbm = take(2)
    tables = take(8)
    before_hbm = [] if first_call else take(2)
    (held_hbm,), sums_hbm = take(1), take(2)
    own_ref, vis_ref, real_ref, imag_ref, weights_ref, total_ref, other_ref = take(7)
    own_sem, vis_sem, near_sem, weights_sem, before_sem, held_sem, sums_sem = take(7)
    send_sem, recv_sem, cross_sem, crossed_sem = refs
    nz, ny, _ = real_ref.shape
    depth = nz // 4
    rank = lax.axis_index("grid")
    partner = {"grid": lax.bitwise_xor(rank, 1)}
    barrier = pltpu.get_barrier_semaphore()
    pl.semaphore_signal(barrier, inc=1, device_id=partner, device_id_type=MESH)

    def base(slot):
        return lax.bitwise_xor(rank, slot) * depth

    own_in, vis_in, near_in, before_in, far_in = [], [], [], [], []
    half = depth // 2
    for s in range(2):
        here, part = pl.ds(base(s), depth), pl.ds(s * depth, depth)
        own_in.append(pltpu.make_async_copy(own_hbm[s], own_ref.at[:, here], own_sem.at[s, 0]))
        vis_in.append(pltpu.make_async_copy(vis_hbm[s], vis_ref.at[here], vis_sem.at[s, 0]))
        for i, ref in enumerate((real_ref, imag_ref)):
            near_in.append(
                pltpu.make_async_copy(near_hbm.at[i, part], ref.at[here], near_sem.at[s, i])
            )
        if not first_call:
            before_in.append(
                pltpu.make_async_copy(before_hbm[s], total_ref.at[:, part], before_sem.at[s])
            )
    for s in range(2, 4):
        for h in range(2):
            here, part = pl.ds(base(s) + h * half, half), pl.ds(h * half, half)
            far_in.append(
                [
                    pltpu.make_async_copy(
                        own_hbm[s].at[:, part], own_ref.at[:, here], own_sem.at[s, h]
                    )
                ]
            )
            if s == 2:
                far_in[-1].append(
                    pltpu.make_async_copy(
                        vis_hbm[s].at[part], vis_ref.at[here], vis_sem.at[s, h]
                    )
                )
    stripes = weights_sem.shape[0]
    stripe = ny // stripes
    weights_in = []
    for i in range(stripes):
        part = pl.ds(i * stripe, stripe)
        weights_in.append(
            pltpu.make_async_copy(
                weights_hbm.at[:, part], weights_ref.at[:, part], weights_sem.at[i]
            )
        )

    def start(copies):
        for copy in copies:
            copy.start()

    def crossing(h):
        return pltpu.make_async_remote_copy(
            src_ref=vis_hbm[2].at[pl.ds(h * half, half)],
            dst_ref=vis_ref.at[pl.ds(base(2) + h * half, half)],
            send_sem=cross_sem.at[h],
            recv_sem=crossed_sem.at[h],
            device_id=partner,
            device_id_type=MESH,
        )

    start(far_in[0])
    pl.semaphore_wait(barrier, 1)
    start([crossing(0), crossing(1)])

    def loaded(index):
        return tables[index][...], tables[index + 1][...]

    def forward(z):
        here = pl.ds(z, 2)
        visitor = vis_ref[here]
        real, imag = transform_planes(
            own_ref[0, here] * visitor, own_ref[1, here] * visitor, loaded(0), loaded(2), False
        )
        real_ref[here] = real
        imag_ref[here] = imag

    def backward(z, kept, other):
        here = pl.ds(z, 2)
        real, imag = transform_planes(real_ref[here], imag_ref[here], loaded(6), loaded(4), True)
        visitor = vis_ref[here]
        held = real * own_ref[0, here] + imag * own_ref[1, here]
        vis_ref[here] = held if other is None else held + other_ref[pl.ds(other, 2)]
        for i, part in enumerate((real, imag)):
            part = part * visitor
            if not first_call:
                part = part + total_ref[i, pl.ds(kept, 2)]
            total_ref[i, pl.ds(kept, 2)] = part

    def tile(index, carry):
        here = pl.ds(pl.multiple_of(8 * index, 8), 8)
        outer = nz // radix

        def load(z):
            return real_ref[z, here, :], imag_ref[z, here, :]

        def store(z, value):
            real_ref[z, here, :], imag_ref[z, here, :] = value

        for fine in range(radix):
            values = fourier([load(radix * n + fine) for n in range(outer)], -1.0)
            for k, value in enumerate(values):
                store(radix * k + fine, times(value, turn(fine * k, nz, -1.0)))
        for k in range(outer):
            values = fourier([load(radix * k + n) for n in range(radix)], -1.0)
            for n, (a, b) in enumerate(values):
                weight = weights_ref[radix * k + n, here, :]
                values[n] = (a * weight, b * weight)
            for n, value in enumerate(fourier(values, 1.0)):
                store(radix * k + n, value)
        for fine in range(radix):
            values = [times(load(radix * k + fine), turn(fine * k, nz, 1.0)) for k in range(outer)]
            for n, value in enumerate(fourier(values, 1.0)):
                store(radix * n + fine, value)
        return carry

    per_slot = depth // CHUNK

    def arrived(copies):
        for copy in copies:
            copy.wait()

    arrived(far_in[0])
    start(far_in[1] + near_in[:2])

    def forward_chunk(index, carry):
        per_half = per_slot // 2
        for h, later in (
            (1, far_in[2] + near_in[2:]),
            (2, far_in[3] + weights_in[:1]),
            (3, weights_in[1:]),
        ):

            @pl.when(index == h * per_half)
            def _():
                arrived(far_in[h])
                if h >= 2:
                    crossing(h - 2).wait_recv()
                start(later)

        first = base(2 + index // per_slot) + index % per_slot * CHUNK
        for pair in range(CHUNK // 2):
            forward(first + 2 * pair)
        return carry

    lax.fori_loop(0, 2 * per_slot, forward_chunk, 0)
    arrived(near_in)

    def tile_and_wait(index, carry):
        for i in range(stripes):

            @pl.when(index == i * (stripe // 8))
            def _():
                arrived(weights_in[i : i + 1])
                if i == 1:
                    start(own_in[1::-1] + vis_in[1::-1] + before_in)

        return tile(index, carry)

    lax.fori_loop(0, ny // 8, tile_and_wait, 0)
    arrived(own_in + vis_in + before_in)

    def sent(index):
        part = pl.ds(index * CHUNK, CHUNK)
        return pltpu.make_async_remote_copy(
            src_ref=vis_ref.at[pl.ds(base(1) + index * CHUNK, CHUNK)],
            dst_ref=other_ref.at[part],
            send_sem=send_sem.at[index],
            recv_sem=recv_sem.at[index],
            device_id=partner,
            device_id_type=MESH,
        )

    def summed(slot, index):
        part = pl.ds(index * CHUNK, CHUNK)
        return pltpu.make_async_copy(
            total_ref.at[:, pl.ds(slot * depth + index * CHUNK, CHUNK)],
            sums_hbm[slot].at[:, part],
            sums_sem.at[slot],
        )

    def for_partner(index, carry):
        for pair in range(CHUNK // 2):
            offset = index * CHUNK + 2 * pair
            backward(base(1) + offset, depth + offset, None)
        sent(index).start()
        summed(1, index).start()
        return carry

    def for_self(index, carry):
        sent(index).wait_recv()
        for pair in range(CHUNK // 2):
            offset = index * CHUNK + 2 * pair
            backward(base(0) + offset, offset, offset)
        pltpu.make_async_copy(
            vis_ref.at[pl.ds(base(0) + index * CHUNK, CHUNK)],
            held_hbm.at[pl.ds(index * CHUNK, CHUNK)],
            held_sem,
        ).start()
        summed(0, index).start()
        return carry

    def left(index, carry):
        sent(index).wait_send()
        return carry

    lax.fori_loop(0, per_slot, for_partner, 0)
    lax.fori_loop(0, per_slot, for_self, 0)
    lax.fori_loop(0, per_slot, left, 0)
    for h in range(2):
        crossing(h).wait_send()
    pltpu.make_async_copy(vis_ref.at[pl.ds(base(0), depth)], held_hbm, held_sem).wait()
    for s in range(2):
        pltpu.make_async_copy(
            total_ref.at[:, pl.ds(s * depth, depth)], sums_hbm[s], sums_sem.at[s]
        ).wait()


def solve_field(owned, visitor, near, weights, tables, before):
    depth, ny, nx = visitor[0].shape
    nz = 4 * depth
    first_call = before is None
    operands = list(owned) + list(visitor) + [near, weights] + list(tables)
    anywhere = pl.BlockSpec(memory_space=pl.ANY)
    in_specs = [anywhere] * 9
    in_specs += [pl.BlockSpec(memory_space=pltpu.VMEM)] * 8
    if not first_call:
        in_specs += [anywhere] * 2
        operands += list(before)
    shapes = [jax.ShapeDtypeStruct(v.shape, v.dtype) for v in [visitor[0], *owned[:2]]]
    points = nz * ny * nx
    grid = pltpu.VMEM((nz, ny, nx), jnp.float32)
    results = pl.pallas_call(
        functools.partial(field_kernel, 8, first_call),
        out_shape=shapes,
        in_specs=in_specs,
        out_specs=[anywhere] * 3,
        scratch_shapes=[
            pltpu.VMEM((2, nz, ny, nx), jnp.float32),
            grid,
            grid,
            grid,
            grid,
            pltpu.VMEM((2, 2 * depth, ny, nx), jnp.float32),
            pltpu.VMEM((depth, ny, nx), jnp.float32),
            pltpu.SemaphoreType.DMA((4, 2)),
            pltpu.SemaphoreType.DMA((4, 2)),
            pltpu.SemaphoreType.DMA((2, 2)),
            pltpu.SemaphoreType.DMA((4,)),
            pltpu.SemaphoreType.DMA((2,)),
            pltpu.SemaphoreType.DMA,
            pltpu.SemaphoreType.DMA((2,)),
            pltpu.SemaphoreType.DMA((depth // CHUNK,)),
            pltpu.SemaphoreType.DMA((depth // CHUNK,)),
            pltpu.SemaphoreType.DMA((2,)),
            pltpu.SemaphoreType.DMA((2,)),
        ],
        compiler_params=pltpu.CompilerParams(
            vmem_limit_bytes=67043328,
            collective_id=0 if first_call else 1,
            has_side_effects=True,
        ),
        cost_estimate=pl.CostEstimate(
            flops=2 * points * 3 * 4 * nx, bytes_accessed=4 * points * 10, transcendentals=0
        ),
        name="solve_field",
    )(*operands)
    return results[0], results[1:]


def place_kernel(place, _, row, out, sem):
    copy = pltpu.make_async_copy(row, out.at[place], sem)
    copy.start()
    copy.wait()


def placed_row(rows, row, place):
    anywhere = pl.BlockSpec(memory_space=pl.ANY)
    return pl.pallas_call(
        functools.partial(place_kernel, place),
        out_shape=jax.ShapeDtypeStruct(rows.shape, rows.dtype),
        in_specs=[anywhere, pl.BlockSpec(memory_space=pltpu.VMEM)],
        out_specs=anywhere,
        scratch_shapes=[pltpu.SemaphoreType.DMA],
        input_output_aliases={0: 0},
        compiler_params=pltpu.CompilerParams(vmem_limit_bytes=50 * 1024 * 1024),
        name="place_row",
    )(rows, row)


def exchanged(block, bit):
    devices = range(lax.axis_size("grid"))
    return lax.ppermute(block, "grid", [(i, i ^ bit) for i in devices])


def picked(bands, first, count):
    return lax.dynamic_slice_in_dim(bands, first, count, 0)


def square_body(own_bands, travel_bands):
    rank = lax.axis_index("grid")
    core = rank % 2
    half_own = own_bands.shape[0] // 2
    count_vis = travel_bands.shape[0]
    depth, ny, nx = own_bands.shape[1:]
    nz = depth * lax.axis_size("grid")

    own_mine = picked(own_bands, core * half_own, half_own)
    own_far = exchanged(own_mine, 2)
    own_bands, travel_bands, _ = lax.optimization_barrier((own_bands, travel_bands, own_mine))
    own_side = exchanged(picked(own_bands, (1 - core) * half_own, half_own), 1)
    own_cross = exchanged(own_side, 2)
    owned = [own_mine, own_side, own_far, own_cross]

    visitors = []
    for j in range(count_vis):
        near = passed_along(travel_bands[j], "band", 1)
        far = exchanged(near, 2)
        side = exchanged(near, 1)
        visitors.append([near, side, far])

    radix = 8
    slot = jnp.arange(nz, dtype=jnp.int32)
    z_of_slot = slot // radix + (nz // radix) * (slot % radix)
    weights = (-FRACTION / (nz * ny * nx)) * coulomb(
        squared_wavenumber(z_of_slot, nz), wave_square(ny, 0, ny), wave_square(nx, 0, nx)
    )
    tables = []
    for length, inverse, left in (
        (nx, False, False),
        (ny, False, True),
        (ny, True, True),
        (nx, True, False),
    ):
        tables += halves(complex_matrix(length, inverse, left))

    nears = []
    for j in range(count_vis):
        order = nears[-1] if nears else weights
        nears.append(near_field(owned, visitors[j], order, tables))

    sums = None
    returned = []
    for j in range(count_vis):
        held, sums = solve_field(owned, visitors[j], nears[j], weights, tables, sums)
        returned.append(passed_along(held, "band", -1))

    own_other = exchanged(sums[1], 1)
    own_rows = jnp.zeros(own_bands.shape, own_bands.dtype)
    own_rows = lax.dynamic_update_slice_in_dim(own_rows, sums[0], core * half_own, 0)
    own_rows = lax.dynamic_update_slice_in_dim(own_rows, own_other, (1 - core) * half_own, 0)
    held_rows = jnp.zeros(travel_bands.shape, travel_bands.dtype)
    for j in range(count_vis - 1):
        held_rows = lax.dynamic_update_slice_in_dim(held_rows, returned[j][None], j, 0)
    held_rows = placed_row(held_rows, returned[-1], count_vis - 1)
    return own_rows, held_rows


def whole_body(own_bands, travel_bands):
    return square_body(own_bands, travel_bands)


def solution(mesh):
    spec = P("band", "grid", None, None)

    def placed(own_bands, travel_bands):
        group_own = own_bands.shape[0] // mesh.shape["band"]
        group_vis = travel_bands.shape[0] // mesh.shape["band"]
        square = mesh.shape["grid"] == 4 and group_own == 4 and group_vis % 2 == 0
        step = jax.shard_map(
            whole_body if square else body,
            mesh=mesh,
            in_specs=(spec, spec),
            out_specs=(spec, spec),
            check_vma=False,
        )
        return step(own_bands, travel_bands)

    return placed
```
